8 devices in a mesh: dp: 2 (over y, z), sp: 4 (over x, core).
Axes of the slice: x: 2, y: 2, z: 1, core: 2. Of those that a mesh axis runs over, the one named last changes fastest.
Arguments:
- x: bfloat16 [8192, 2560], P(('dp', 'sp')), parts along dimension 0
- gain: bfloat16 [2560], replicated
- wq: bfloat16 [2560, 4096], P('sp')
- wk: bfloat16 [2560, 1024], P('sp')
- wv: bfloat16 [2560, 1024], P('sp')
- wo: bfloat16 [4096, 2560], P('sp')
Outputs:
- output: bfloat16 [8192, 2560], P(('dp', 'sp')), parts along dimension 0
There are 2 independent parts. The reference program is written for one: setup_inputs(seed, part) draws one part's arguments, and reference() takes and returns one part's arrays. A program takes and returns all parts, laid end to end along the dimension named above; an argument that names none is the same for every part.
All inputs are finite; a program needn't handle non-finite values.
Results may differ from the reference program's by a relative error of at most 0.012.
Values are sent between devices in bfloat16 or wider.
A program may use at most 2 GiB of HBM per device.

```python
import jax
import jax.numpy as jnp
from jax import lax

ROWS = 4096
D = 2560
HEADS = 32
KV_HEADS = 8
HEAD = 128
THETA = 10000


def setup_inputs(seed: int = 0, part: int = 0) -> dict:
    kx, kn, kq, kk, kv, ko = jax.random.split(jax.random.key(seed), 6)

    def weights(key, rows, columns):
        return jax.random.normal(key, (rows, columns), jnp.float32) * rows**-0.5

    drawn = {
        "x": jax.random.normal(jax.random.fold_in(kx, part), (ROWS, D), jnp.float32),
        "gain": 1 + 0.1 * jax.random.normal(kn, (D,), jnp.float32),
        "wq": 2 * weights(kq, D, HEADS * HEAD),
        "wk": 2 * weights(kk, D, KV_HEADS * HEAD),
        "wv": 4 * weights(kv, D, KV_HEADS * HEAD),
        "wo": weights(ko, HEADS * HEAD, D),
    }
    return {k: v.astype(jnp.bfloat16) for k, v in drawn.items()}


def normed(x, gain):
    wide = x.astype(jnp.float32)
    scale = lax.rsqrt(jnp.mean(wide * wide, -1, keepdims=True) + 1e-6)
    return (wide * scale * gain.astype(jnp.float32)).astype(jnp.bfloat16)


def turned(t, place, theta):
    half = t.shape[-1] // 2
    angle = place.astype(jnp.float32)[:, None] * theta ** (-jnp.arange(half, dtype=jnp.float32) / half)
    cos, sin = jnp.cos(angle)[:, None], jnp.sin(angle)[:, None]
    a, b = t[..., :half].astype(jnp.float32), t[..., half:].astype(jnp.float32)
    return jnp.concatenate([a * cos - b * sin, b * cos + a * sin], -1).astype(jnp.bfloat16)


def matmul(a, w):
    return jnp.dot(a, w, preferred_element_type=jnp.float32).astype(jnp.bfloat16)


def einsum(form, a, b):
    return jnp.einsum(form, a.astype(jnp.float32), b.astype(jnp.float32))


def attention(q, k, v):
    scores = einsum("tgsd,ugd->gstu", q, k) * q.shape[-1] ** -0.5
    token = jnp.arange(q.shape[0])
    scores = jnp.where(token[:, None] >= token, scores, -jnp.inf)
    weights = jax.nn.softmax(scores, -1).astype(jnp.bfloat16)
    return einsum("gstu,ugd->tgsd", weights, v).astype(jnp.bfloat16)


def reference(x, gain, wq, wk, wv, wo):
    a, place = normed(x, gain), jnp.arange(ROWS)
    q = turned(matmul(a, wq).reshape(ROWS, HEADS, HEAD), place, THETA).reshape(ROWS, KV_HEADS, -1, HEAD)
    k = turned(matmul(a, wk).reshape(ROWS, KV_HEADS, HEAD), place, THETA)
    v = matmul(a, wv).reshape(ROWS, KV_HEADS, HEAD)
    seen = attention(q, k, v).reshape(ROWS, HEADS * HEAD)
    return (x.astype(jnp.float32) + jnp.dot(seen, wo, preferred_element_type=jnp.float32)).astype(jnp.bfloat16)
```

```python
import functools

import jax
import jax.numpy as jnp
import numpy as np
from jax import lax
from jax.experimental import pallas as pl
from jax.experimental.pallas import tpu as pltpu
from jax.sharding import PartitionSpec as P

HEAD = 128
THETA = 10000
NEG = -1e30
HIDDEN = 2 * NEG
LOG2E = 1.4426950408889634
D = 2560
OWN = 1024
CHIP = 2 * OWN
STEPS = 4
G = 4
QC = G * HEAD
WC = QC + 2 * HEAD
SHARD = D // 4
HALF = SHARD // 2
BQ = 512
BK = 512
COLS = G * BQ
VR = HEAD + 16
SUB = 128
MESH = pl.DeviceIdType.MESH


def _dot(a, b, ca, cb):
    return lax.dot_general(a, b, (((ca,), (cb,)), ((), ())), preferred_element_type=jnp.float32)


def _kernel(x_ref, gain_ref, freq_ref, wq_ref, wk_ref, wv_ref, wo_ref, seen_ref, wof_ref,
            a_s, w_s, k_s, v_s, q_s, st_s, cos_s, sin_s, top_s, mix_s,
            lx, a_send, a_recv, lw, sw_send, sw_recv, xw_send, xw_recv, yw_send, yw_recv, kv_send, kv_recv,
            so_loc, so_send, so_recv, lwo, swo_send, swo_recv, wx_send, wx_recv, wy_send, wy_recv,
            wsx_send, wsx_recv, wsy_send, wsy_recv):
    y, s = lax.axis_index("dp"), lax.axis_index("sp")
    chip, c = lax.div(s, 2), lax.rem(s, 2)
    other = 2 * (1 - chip)
    sib = (y, s + 1 - 2 * c)
    across = lambda core: (y, other + core)
    twin = (1 - y, s)
    scale = HEAD**-0.5
    e = scale * LOG2E

    def remote(src, dst, send, recv, device):
        return pltpu.make_async_remote_copy(src_ref=src, dst_ref=dst, send_sem=send, recv_sem=recv, device_id=device, device_id_type=MESH)

    barrier = pltpu.get_barrier_semaphore()
    for device in (sib, across(0), across(1), twin):
        pl.semaphore_signal(barrier, inc=1, device_id=device, device_id_type=MESH)
    pl.semaphore_wait(barrier, 4)

    def pieces(core, j, row, n):
        h = 2 * j + core
        rows = pl.ds(row, n)
        return ((wq_ref.at[rows, pl.ds(pl.multiple_of(h * QC, QC), QC)], pl.ds(0, QC)),
                (wk_ref.at[rows, pl.ds(pl.multiple_of(h * HEAD, HEAD), HEAD)], pl.ds(QC, HEAD)),
                (wv_ref.at[rows, pl.ds(pl.multiple_of(h * HEAD, HEAD), HEAD)], pl.ds(QC + HEAD, HEAD)))

    def place(j, row, n):
        return w_s.at[j, pl.ds(pl.multiple_of(row, HALF), n), :]

    def w_local(j):
        for src, cols in pieces(c, j, 0, SHARD):
            pltpu.make_async_copy(src, w_s.at[j, pl.ds(pl.multiple_of(s * SHARD, HALF), SHARD), cols], lw.at[j]).start()

    def w_sib(j):
        for src, cols in pieces(1 - c, j, 0, SHARD):
            remote(src, w_s.at[j, pl.ds(pl.multiple_of(s * SHARD, HALF), SHARD), cols], sw_send.at[j], sw_recv.at[j], sib).start()

    def w_across(j):
        for core in range(2):
            row = pl.multiple_of(y * HALF, HALF)
            for src, cols in pieces(core, j, row, HALF):
                remote(src, w_s.at[j, pl.ds(pl.multiple_of(s * SHARD + y * HALF, HALF), HALF), cols],
                       xw_send.at[j, core], xw_recv.at[j, c], across(core)).start()

    def w_forward(j):
        for core in range(2):
            here = place(j, (other + core) * SHARD + y * HALF, HALF)
            remote(here, here, xw_send.at[j, core], xw_recv.at[j, core], across(core)).wait_recv()
            remote(here, here, yw_send.at[j, core], yw_recv.at[j, core], twin).start()

    def w_wait(j):
        here = place(j, s * SHARD, SHARD)
        pltpu.make_async_copy(here, here, lw.at[j]).wait()
        here = place(j, (s + 1 - 2 * c) * SHARD, SHARD)
        remote(here, here, sw_send.at[j], sw_recv.at[j], sib).wait_recv()
        for core in range(2):
            here = place(j, (other + core) * SHARD + (1 - y) * HALF, HALF)
            remote(here, here, yw_send.at[j, core], yw_recv.at[j, core], twin).wait_recv()

    def wo_rows(owner, quarter, k):
        return pl.ds(pl.multiple_of(owner * OWN + quarter * 256 + k * SUB, SUB), SUB)

    def wo_across(k):
        for core in range(2):
            src = wo_ref.at[pl.ds(pl.multiple_of((2 * y + core) * 256 + k * SUB, SUB), SUB), :]
            remote(src, wof_ref.at[wo_rows(s, 2 * y + core, k), :], wx_send.at[k, core], wx_recv.at[k, c], across(core)).start()

    def wo_forward(k):
        for core in range(2):
            here = wof_ref.at[wo_rows(other + core, 2 * y + c, k), :]
            remote(here, here, wx_send.at[k, core], wx_recv.at[k, core], across(core)).wait_recv()
            remote(here, here, wy_send.at[k, core], wy_recv.at[k, core], twin).start()
            remote(here, here, wsx_send.at[k, core], wsx_recv.at[k, core], sib).start()

    def wo_share(k):
        for core in range(2):
            here = wof_ref.at[wo_rows(other + core, 2 * (1 - y) + c, k), :]
            remote(here, here, wy_send.at[k, core], wy_recv.at[k, core], twin).wait_recv()
            remote(here, here, wsy_send.at[k, core], wsy_recv.at[k, core], sib).start()

    w_across(0)
    w_local(0)
    w_sib(0)
    w_across(1)
    for i in range(4):
        rows = pl.ds(pl.multiple_of(c * OWN + i * 256, 256), 256)
        pltpu.make_async_copy(x_ref.at[pl.ds(i * 256, 256), :], a_s.at[rows, :], lx.at[i]).start()

    @pl.loop(0, CHIP // 256)
    def _(i):
        rows = pl.ds(pl.multiple_of(i * 256, 256), 256)
        spot = (chip * CHIP + i * 256 + lax.broadcasted_iota(jnp.int32, (256, HEAD), 0)).astype(jnp.float32)
        angle = spot * freq_ref[...]
        cos_s[rows, :] = jnp.cos(angle)
        left = lax.broadcasted_iota(jnp.int32, (256, HEAD), 1) < HEAD // 2
        sin = jnp.sin(angle)
        sin_s[rows, :] = jnp.where(left, -sin, sin)

    gain = gain_ref[...].astype(jnp.float32)

    def a_rows(core, i):
        return a_s.at[pl.ds(pl.multiple_of(core * OWN + i * 256, 256), 256), :]

    def a_copy(core, i):
        return remote(a_rows(core, i), a_rows(core, i), a_send.at[i], a_recv.at[i], sib)

    for i in range(4):
        pltpu.make_async_copy(x_ref.at[pl.ds(i * 256, 256), :], a_rows(c, i), lx.at[i]).wait()

        @pl.loop(0, 256 // 32)
        def _(r):
            rows = pl.ds(pl.multiple_of(c * OWN + i * 256 + r * 32, 32), 32)
            wide = a_s[rows, :].astype(jnp.float32)
            inverse = lax.rsqrt(jnp.mean(wide * wide, -1, keepdims=True) + 1e-6)
            a_s[rows, :] = (wide * inverse * gain).astype(jnp.bfloat16)

        if i:
            a_copy(c, i - 1).start()
    for j in range(1, STEPS):
        w_local(j)
    v_s[:, :, HEAD:, :] = jnp.ones((STEPS, 2, VR - HEAD, CHIP), jnp.bfloat16)
    a_copy(c, 3).start()
    for j in range(1, STEPS):
        w_sib(j)
    w_forward(0)
    for i in range(4):
        a_copy(1 - c, i).wait_recv()

    def project(t):
        slot = lax.rem(t, 2)

        @pl.loop(0, CHIP // 512)
        def _(m):
            rows = pl.ds(pl.multiple_of(m * 512, 512), 512)
            got = _dot(a_s[rows, :], w_s[t], 1, 0)
            cos, sin = cos_s[rows, :], sin_s[rows, :]
            for g in range(G + 1):
                part = got[:, g * HEAD : (g + 1) * HEAD].astype(jnp.bfloat16).astype(jnp.float32)
                part = (part * cos + pltpu.roll(part, HEAD // 2, 1) * sin).astype(jnp.bfloat16)
                if g < G:
                    q_s[slot, g, rows, :] = part
                else:
                    k_s[t, chip, rows, :] = part
            v_s[t, chip, :HEAD, rows] = got[:, QC + HEAD :].T.astype(jnp.bfloat16)

    def kv_copies(t):
        k, v = k_s.at[t, 0], v_s.at[t, 0, :HEAD, :]
        device = (y, 2 * (1 - chip) + c)
        return remote(k, k, kv_send.at[t, 0], kv_recv.at[t, 0], device), remote(v, v, kv_send.at[t, 1], kv_recv.at[t, 1], device)

    def seen_place(j, iq):
        return seen_ref.at[pl.ds(pl.multiple_of(lax.rem(iq, 2) * BQ, BQ), BQ), pl.ds(pl.multiple_of((2 * j + c) * QC, QC), QC)]

    def seen_remote(j, iq):
        return remote(st_s.at[j, iq], seen_place(j, iq), so_send.at[j, iq], so_recv.at[j, iq], sib)

    def seen_local(j, iq):
        return pltpu.make_async_copy(st_s.at[j, iq], seen_place(j, iq), so_loc.at[j, iq])

    def attend(j):
        slot = lax.rem(j, 2)

        @pl.loop(0, CHIP // BQ)
        def _(iq):
            queries = pl.ds(pl.multiple_of(iq * BQ, BQ), BQ)

            def block(half, at, first):
                here = pl.ds(pl.multiple_of(at * BK, BK), BK)
                keys = k_s[j, half, here, :]
                scores = [_dot(keys, q_s[slot, g, queries, :], 1, 1) for g in range(G)]
                weights, keeps = [], []
                for g, sc in enumerate(scores):
                    cols = slice(g * BQ, (g + 1) * BQ)
                    if first:
                        ok = lax.broadcasted_iota(jnp.int32, (BK, BQ), 1) >= lax.broadcasted_iota(jnp.int32, (BK, BQ), 0)
                        sc = jnp.where(ok, sc, HIDDEN)
                        top = sc.max(axis=0, keepdims=True)
                    else:
                        old = top_s[:, cols]
                        top = jnp.maximum(old, sc.max(axis=0, keepdims=True))
                        keeps.append(jnp.exp2((old - top) * e))
                    top_s[:, cols] = top
                    weights.append(jnp.exp2((sc - top) * e).astype(jnp.bfloat16))
                values = v_s[j, half, :, here]
                for g, p in enumerate(weights):
                    cols = slice(g * BQ, (g + 1) * BQ)
                    new = _dot(values, p, 1, 0)
                    mix_s[:, cols] = new if first else mix_s[:, cols] * keeps[g] + new

            block(chip, iq, True)

            @pl.when((iq == 0) & (chip == 1))
            def _():
                for copy in kv_copies(j):
                    copy.wait_recv()

            @pl.loop(0, iq + chip * (CHIP // BK))
            def _(i):
                own = i < iq
                block(jnp.where(own, chip, 0), jnp.where(own, i, i - iq), False)

            for g in range(G):
                cols = slice(g * BQ, (g + 1) * BQ)
                total = mix_s[HEAD : HEAD + 1, cols]
                st_s[j, iq, :, g * HEAD : (g + 1) * HEAD] = (mix_s[:HEAD, cols] * (1 / total)).T.astype(jnp.bfloat16)

            @pl.when(lax.div(iq, 2) == c)
            def _():
                seen_local(j, iq).start()

            @pl.when(lax.div(iq, 2) != c)
            def _():
                seen_remote(j, iq).start()

            @pl.when((iq == 2) & (j < 2))
            def _():
                w_forward(j + 2)

            @pl.when((iq == 2) & (j >= 2))
            def _():
                wo_forward(j - 2)

            @pl.when((iq == 3) & (j == 3))
            def _():
                wo_share(0)

    @pl.loop(0, STEPS + 1)
    def _(t):
        @pl.when(t < STEPS)
        def _():
            w_wait(t)
            project(t)

            @pl.when(chip == 0)
            def _():
                for copy in kv_copies(t):
                    copy.start()

            @pl.when(t == 0)
            def _():
                w_across(2)
                w_forward(1)
                remote(wo_ref, wof_ref.at[pl.ds(pl.multiple_of(s * OWN, OWN), OWN), :], swo_send, swo_recv, sib).start()
                pltpu.make_async_copy(wo_ref, wof_ref.at[pl.ds(pl.multiple_of(s * OWN, OWN), OWN), :], lwo).start()

            @pl.when(t == 1)
            def _():
                w_across(3)

            @pl.when(t >= 2)
            def _():
                wo_across(t - 2)

        @pl.when(t > 0)
        def _():
            attend(t - 1)

    wo_share(1)
    mine = wof_ref.at[pl.ds(pl.multiple_of(s * OWN, OWN), OWN), :]
    pltpu.make_async_copy(wo_ref, mine, lwo).wait()
    theirs = wof_ref.at[pl.ds(pl.multiple_of((s + 1 - 2 * c) * OWN, OWN), OWN), :]
    remote(wo_ref, mine, swo_send, swo_recv, sib).wait_send()
    remote(theirs, theirs, swo_send, swo_recv, sib).wait_recv()
    for i in range(4):
        a_copy(c, i).wait_send()
    for j in range(STEPS):
        here = place(j, s * SHARD, SHARD)
        remote(here, here, sw_send.at[j], sw_recv.at[j], sib).wait_send()
        for core in range(2):
            here = place(j, s * SHARD + y * HALF, HALF)
            remote(here, here, xw_send.at[j, core], xw_recv.at[j, c], across(core)).wait_send()
            here = place(j, (other + core) * SHARD + y * HALF, HALF)
            remote(here, here, yw_send.at[j, core], yw_recv.at[j, core], twin).wait_send()

        @pl.when(chip == 0)
        def _():
            for copy in kv_copies(j):
                copy.wait_send()

        for i in range(2):
            seen_local(j, 2 * c + i).wait()
            seen_remote(j, 2 * (1 - c) + i).wait_send()
            here = seen_ref.at[pl.ds(i * BQ, BQ), pl.ds(pl.multiple_of((2 * j + 1 - c) * QC, QC), QC)]
            remote(here, here, so_send.at[j, 2 * c + i], so_recv.at[j, 2 * c + i], sib).wait_recv()
    for k in range(2):
        for core in range(2):
            mine = wof_ref.at[wo_rows(s, 2 * y + core, k), :]
            remote(mine, mine, wx_send.at[k, core], wx_recv.at[k, c], across(core)).wait_send()
            here = wof_ref.at[wo_rows(other + core, 2 * y + c, k), :]
            remote(here, here, wy_send.at[k, core], wy_recv.at[k, core], twin).wait_send()
            remote(here, here, wsx_send.at[k, core], wsx_recv.at[k, core], sib).wait_send()
            here = wof_ref.at[wo_rows(other + core, 2 * (1 - y) + c, k), :]
            remote(here, here, wsy_send.at[k, core], wsy_recv.at[k, core], sib).wait_send()
            here = wof_ref.at[wo_rows(other + core, 2 * y + 1 - c, k), :]
            remote(here, here, wsx_send.at[k, core], wsx_recv.at[k, core], sib).wait_recv()
            here = wof_ref.at[wo_rows(other + core, 2 * (1 - y) + 1 - c, k), :]
            remote(here, here, wsy_send.at[k, core], wsy_recv.at[k, core], sib).wait_recv()


def _gather_and_attend(x, gain, freq, wq, wk, wv, wo):
    dma = lambda *shape: pltpu.SemaphoreType.DMA(shape) if shape else pltpu.SemaphoreType.DMA
    hbm, vmem = pl.BlockSpec(memory_space=pl.ANY), pl.BlockSpec(memory_space=pltpu.VMEM)
    bf16, f32 = jnp.bfloat16, jnp.float32
    return pl.pallas_call(
        _kernel,
        out_shape=[jax.ShapeDtypeStruct((OWN, 4 * OWN), bf16), jax.ShapeDtypeStruct((4 * OWN, D), bf16)],
        in_specs=[hbm, vmem, vmem, hbm, hbm, hbm, hbm],
        out_specs=[hbm, hbm],
        scratch_shapes=[
            pltpu.VMEM((CHIP, D), bf16), pltpu.VMEM((STEPS, D, WC), bf16), pltpu.VMEM((STEPS, 2, CHIP, HEAD), bf16),
            pltpu.VMEM((STEPS, 2, VR, CHIP), bf16), pltpu.VMEM((2, G, CHIP, HEAD), bf16), pltpu.VMEM((STEPS, CHIP // BQ, BQ, QC), bf16),
            pltpu.VMEM((CHIP, HEAD), f32), pltpu.VMEM((CHIP, HEAD), f32), pltpu.VMEM((1, COLS), f32), pltpu.VMEM((VR, COLS), f32),
            dma(4), dma(4), dma(4), dma(4), dma(4), dma(4), dma(4, 2), dma(4, 2), dma(4, 2), dma(4, 2), dma(4, 2), dma(4, 2),
            dma(4, 4), dma(4, 4), dma(4, 4), dma(), dma(), dma(), dma(2, 2), dma(2, 2), dma(2, 2), dma(2, 2),
            dma(2, 2), dma(2, 2), dma(2, 2), dma(2, 2),
        ],
        compiler_params=pltpu.CompilerParams(collective_id=0, has_side_effects=True, vmem_limit_bytes=63 * 2**20),
        cost_estimate=pl.CostEstimate(flops=120 * 10**9, transcendentals=10**8, bytes_accessed=100 * 2**20),
    )(x, gain, freq, wq, wk, wv, wo)


def solution(mesh):
    def step(x, gain, wq, wk, wv, wo):
        half = HEAD // 2
        freq = THETA ** (-jnp.arange(half, dtype=jnp.float32) / half)
        freq = jnp.concatenate([freq, freq])[None]
        seen, whole = _gather_and_attend(x, gain[None], freq, wq, wk, wv, wo)
        y = jnp.dot(seen, whole, preferred_element_type=jnp.float32)
        return (x.astype(jnp.float32) + y).astype(jnp.bfloat16)

    tokens, rows = P(("dp", "sp"), None), P("sp", None)
    return jax.shard_map(
        step,
        mesh=mesh,
        in_specs=(tokens, P(None), rows, rows, rows, rows),
        out_specs=tokens,
        check_vma=False,
    )
```

```python
import functools

import jax
import jax.numpy as jnp
from jax import lax
from jax.experimental import pallas as pl
from jax.experimental.pallas import tpu as pltpu
from jax.sharding import PartitionSpec as P

HEAD = 128
THETA = 10000
NEG = -1e30
HIDDEN = 2 * NEG
LOG2E = 1.4426950408889634
D = 2560
OWN = 1024
CHIP = 2 * OWN
STEPS = 4
G = 4
QC = G * HEAD
WC = QC + 2 * HEAD
SHARD = D // 4
HALF = SHARD // 2
CUT = 2
PIECE = HALF // CUT
BQ = 512
BK = 512
COLS = G * BQ
SQ = 256
VR = HEAD + 16
SUB = 32
PARTS = 4
KP = 256 // SUB
MESH = pl.DeviceIdType.MESH


def _dot(a, b, ca, cb):
    return lax.dot_general(a, b, (((ca,), (cb,)), ((), ())), preferred_element_type=jnp.float32)


def _kernel(x_ref, gain_ref, freq_ref, wq_ref, wk_ref, wv_ref, wo_ref, seen_ref, wof_ref,
            a_s, w_s, k_s, v_s, q_s, st_s, cos_s, sin_s, top_s, mix_s,
            lx, a_send, a_recv, lw, sw_send, sw_recv, xw_send, xw_recv, yw_send, yw_recv, kv_send, kv_recv,
            so_loc, so_send, so_recv, lwo, swo_send, swo_recv, wx_send, wx_recv, wy_send, wy_recv,
            wsx_send, wsx_recv, wsy_send, wsy_recv):
    y, s = lax.axis_index("dp"), lax.axis_index("sp")
    chip, c = lax.div(s, 2), lax.rem(s, 2)
    other = 2 * (1 - chip)
    sib = (y, s + 1 - 2 * c)
    across = lambda core: (y, other + core)
    twin = (1 - y, s)
    scale = HEAD**-0.5
    e = scale * LOG2E

    def remote(src, dst, send, recv, device):
        return pltpu.make_async_remote_copy(src_ref=src, dst_ref=dst, send_sem=send, recv_sem=recv, device_id=device, device_id_type=MESH)

    barrier = pltpu.get_barrier_semaphore()
    for device in (sib, across(0), across(1), twin):
        pl.semaphore_signal(barrier, inc=1, device_id=device, device_id_type=MESH)
    pl.semaphore_wait(barrier, 4)

    def pieces(core, j, row, n):
        h = 2 * j + core
        rows = pl.ds(row, n)
        return ((wq_ref.at[rows, pl.ds(pl.multiple_of(h * QC, QC), QC)], pl.ds(0, QC)),
                (wk_ref.at[rows, pl.ds(pl.multiple_of(h * HEAD, HEAD), HEAD)], pl.ds(QC, HEAD)),
                (wv_ref.at[rows, pl.ds(pl.multiple_of(h * HEAD, HEAD), HEAD)], pl.ds(QC + HEAD, HEAD)))

    def place(j, row, n):
        return w_s.at[j, pl.ds(pl.multiple_of(row, 32), n), :]

    def w_local(j):
        for src, cols in pieces(c, j, 0, SHARD):
            pltpu.make_async_copy(src, w_s.at[j, pl.ds(pl.multiple_of(s * SHARD, HALF), SHARD), cols], lw.at[j]).start()

    def w_sib(j):
        for src, cols in pieces(1 - c, j, 0, SHARD):
            remote(src, w_s.at[j, pl.ds(pl.multiple_of(s * SHARD, HALF), SHARD), cols], sw_send.at[j], sw_recv.at[j], sib).start()

    def w_across(j):
        for r in range(CUT):
            for core in range(2):
                row = pl.multiple_of(y * HALF + r * PIECE, 32)
                for src, cols in pieces(core, j, row, PIECE):
                    remote(src, w_s.at[j, pl.ds(pl.multiple_of(s * SHARD + y * HALF + r * PIECE, 32), PIECE), cols],
                           xw_send.at[j, core, r], xw_recv.at[j, c, r], across(core)).start()

    def w_forward(j, r):
        for core in range(2):
            here = place(j, (other + core) * SHARD + y * HALF + r * PIECE, PIECE)
            remote(here, here, xw_send.at[j, core, r], xw_recv.at[j, core, r], across(core)).wait_recv()
            remote(here, here, yw_send.at[j, core, r], yw_recv.at[j, core, r], twin).start()

    def w_wait(j):
        here = place(j, s * SHARD, SHARD)
        pltpu.make_async_copy(here, here, lw.at[j]).wait()
        here = place(j, (s + 1 - 2 * c) * SHARD, SHARD)
        remote(here, here, sw_send.at[j], sw_recv.at[j], sib).wait_recv()
        for core in range(2):
            for r in range(CUT):
                here = place(j, (other + core) * SHARD + (1 - y) * HALF + r * PIECE, PIECE)
                remote(here, here, yw_send.at[j, core, r], yw_recv.at[j, core, r], twin).wait_recv()

    def wo_rows(owner, quarter, k):
        return pl.ds(pl.multiple_of(owner * OWN + quarter * 256 + k * SUB, SUB), SUB)

    def wo_across(k):
        for core in range(2):
            src = wo_ref.at[pl.ds(pl.multiple_of((2 * y + core) * 256 + k * SUB, SUB), SUB), :]
            remote(src, wof_ref.at[wo_rows(s, 2 * y + core, k), :], wx_send.at[k, core], wx_recv.at[k, c], across(core)).start()

    def wo_forward(k):
        for core in range(2):
            here = wof_ref.at[wo_rows(other + core, 2 * y + c, k), :]
            remote(here, here, wx_send.at[k, core], wx_recv.at[k, core], across(core)).wait_recv()
            remote(here, here, wy_send.at[k, core], wy_recv.at[k, core], twin).start()
            remote(here, here, wsx_send.at[k, core], wsx_recv.at[k, core], sib).start()

    def wo_share(k):
        for core in range(2):
            here = wof_ref.at[wo_rows(other + core, 2 * (1 - y) + c, k), :]
            remote(here, here, wy_send.at[k, core], wy_recv.at[k, core], twin).wait_recv()
            remote(here, here, wsy_send.at[k, core], wsy_recv.at[k, core], sib).start()

    w_across(0)
    w_local(0)
    w_sib(0)
    w_across(1)
    for i in range(4):
        rows = pl.ds(pl.multiple_of(c * OWN + i * 256, 256), 256)
        pltpu.make_async_copy(x_ref.at[pl.ds(i * 256, 256), :], a_s.at[rows, :], lx.at[i]).start()

    @pl.loop(0, CHIP // 256)
    def _(i):
        rows = pl.ds(pl.multiple_of(i * 256, 256), 256)
        spot = (chip * CHIP + i * 256 + lax.broadcasted_iota(jnp.int32, (256, HEAD), 0)).astype(jnp.float32)
        angle = spot * freq_ref[...]
        cos_s[rows, :] = jnp.cos(angle)
        left = lax.broadcasted_iota(jnp.int32, (256, HEAD), 1) < HEAD // 2
        sin = jnp.sin(angle)
        sin_s[rows, :] = jnp.where(left, -sin, sin)

    gain = gain_ref[...].astype(jnp.float32)

    def a_rows(core, i):
        return a_s.at[pl.ds(pl.multiple_of(core * OWN + i * 256, 256), 256), :]

    def a_copy(core, i):
        return remote(a_rows(core, i), a_rows(core, i), a_send.at[i], a_recv.at[i], sib)

    for i in range(4):
        pltpu.make_async_copy(x_ref.at[pl.ds(i * 256, 256), :], a_rows(c, i), lx.at[i]).wait()

        @pl.loop(0, 256 // 32)
        def _(r):
            rows = pl.ds(pl.multiple_of(c * OWN + i * 256 + r * 32, 32), 32)
            wide = a_s[rows, :].astype(jnp.float32)
            inverse = lax.rsqrt(jnp.mean(wide * wide, -1, keepdims=True) + 1e-6)
            a_s[rows, :] = (wide * inverse * gain).astype(jnp.bfloat16)

        if i:
            a_copy(c, i - 1).start()
    for j in range(1, STEPS):
        w_local(j)
    v_s[:, :, HEAD:, :] = jnp.ones((STEPS, 2, VR - HEAD, CHIP), jnp.bfloat16)
    a_copy(c, 3).start()
    for j in range(1, STEPS):
        w_sib(j)
    for r in range(CUT):
        w_forward(0, r)
    for i in range(4):
        a_copy(1 - c, i).wait_recv()
    w_forward(1, 0)

    def project(t):
        slot = lax.rem(t, 2)

        @pl.loop(0, CHIP // 512)
        def _(m):
            rows = pl.ds(pl.multiple_of(m * 512, 512), 512)
            got = _dot(a_s[rows, :], w_s[t], 1, 0)
            cos, sin = cos_s[rows, :], sin_s[rows, :]
            for g in range(G + 1):
                part = got[:, g * HEAD : (g + 1) * HEAD].astype(jnp.bfloat16).astype(jnp.float32)
                part = (part * cos + pltpu.roll(part, HEAD // 2, 1) * sin).astype(jnp.bfloat16)
                if g < G:
                    q_s[slot, g, rows, :] = part
                else:
                    k_s[t, chip, rows, :] = part
            v_s[t, chip, :HEAD, rows] = got[:, QC + HEAD :].T.astype(jnp.bfloat16)

    def kv_copies(t):
        k, v = k_s.at[t, 0], v_s.at[t, 0, :HEAD, :]
        device = (y, 2 * (1 - chip) + c)
        return remote(k, k, kv_send.at[t, 0], kv_recv.at[t, 0], device), remote(v, v, kv_send.at[t, 1], kv_recv.at[t, 1], device)

    def seen_place(j, iq):
        return seen_ref.at[pl.ds(pl.multiple_of(lax.rem(iq, 2) * BQ, BQ), BQ), pl.ds(pl.multiple_of((2 * j + c) * QC, QC), QC)]

    def seen_remote(j, iq):
        return remote(st_s.at[j, iq], seen_place(j, iq), so_send.at[j, iq], so_recv.at[j, iq], sib)

    def seen_local(j, iq):
        return pltpu.make_async_copy(st_s.at[j, iq], seen_place(j, iq), so_loc.at[j, iq])

    def queries(iq):
        return pl.ds(pl.multiple_of(iq * BQ, BQ), BQ)

    def block(j, iq, half, at):
        here = pl.ds(pl.multiple_of(at * BK, BK), BK)
        keys = k_s[j, half, here, :]
        scores = [_dot(keys, q_s[lax.rem(j, 2), g, queries(iq), :], 1, 1) for g in range(G)]
        weights, keeps = [], []
        for g, sc in enumerate(scores):
            cols = slice(g * BQ, (g + 1) * BQ)
            old = top_s[iq, :, cols]
            top = jnp.maximum(old, sc.max(axis=0, keepdims=True))
            top_s[iq, :, cols] = top
            keeps.append(jnp.exp2((old - top) * e))
            weights.append(jnp.exp2((sc - top) * e).astype(jnp.bfloat16))
        values = v_s[j, half, :, here]
        for g, p in enumerate(weights):
            cols = slice(g * BQ, (g + 1) * BQ)
            mix_s[iq, :, cols] = mix_s[iq, :, cols] * keeps[g] + _dot(values, p, 1, 0)

    def diagonal(j, iq):
        here = pl.multiple_of(iq * BQ, BQ)
        strips = [(g, at) for g in range(G) for at in range(0, BQ, SQ)]
        scores = [_dot(k_s[j, chip, pl.ds(here, at + SQ), :],
                       q_s[lax.rem(j, 2), g, pl.ds(pl.multiple_of(here + at, SQ), SQ), :], 1, 1) for g, at in strips]
        weights = []
        for (g, at), sc in zip(strips, scores):
            cols = slice(g * BQ + at, g * BQ + at + SQ)
            ok = lax.broadcasted_iota(jnp.int32, sc.shape, 1) + at >= lax.broadcasted_iota(jnp.int32, sc.shape, 0)
            sc = jnp.where(ok, sc, HIDDEN)
            top = sc.max(axis=0, keepdims=True)
            top_s[iq, :, cols] = top
            weights.append(jnp.exp2((sc - top) * e).astype(jnp.bfloat16))
        for (g, at), p in zip(strips, weights):
            mix_s[iq, :, g * BQ + at : g * BQ + at + SQ] = _dot(v_s[j, chip, :, pl.ds(here, at + SQ)], p, 1, 0)

    def attend_own(j):
        @pl.loop(0, CHIP // BQ)
        def _(iq):
            diagonal(j, iq)

            @pl.loop(0, iq)
            def _(i):
                block(j, iq, chip, i)

    def attend_other(j):
        @pl.when(chip == 1)
        def _():
            for copy in kv_copies(j):
                copy.wait_recv()

        @pl.loop(0, CHIP // BQ)
        def _(iq):
            @pl.when((j < 2) & (iq >= CHIP // BQ - CUT))
            def _():
                w_forward(j + 2, iq - (CHIP // BQ - CUT))

            @pl.when(j >= 2)
            def _():
                wo_forward((j - 2) * PARTS + iq)

            @pl.when(j == 3)
            def _():
                wo_share(iq)

            @pl.loop(0, chip * (CHIP // BK))
            def _(i):
                block(j, iq, 0, i)

            for g in range(G):
                cols = slice(g * BQ, (g + 1) * BQ)
                total = mix_s[iq, HEAD : HEAD + 1, cols]
                st_s[j, iq, :, g * HEAD : (g + 1) * HEAD] = (mix_s[iq, :HEAD, cols] * (1 / total)).T.astype(jnp.bfloat16)

            @pl.when(lax.div(iq, 2) == c)
            def _():
                seen_local(j, iq).start()

            @pl.when(lax.div(iq, 2) != c)
            def _():
                seen_remote(j, iq).start()

    @pl.loop(0, STEPS + 1)
    def _(t):
        @pl.when(t < STEPS)
        def _():
            w_wait(t)
            project(t)

            @pl.when(chip == 0)
            def _():
                for copy in kv_copies(t):
                    copy.start()

            @pl.when(t == 0)
            def _():
                w_across(2)
                w_forward(1, 1)
                remote(wo_ref, wof_ref.at[pl.ds(pl.multiple_of(s * OWN, OWN), OWN), :], swo_send, swo_recv, sib).start()
                pltpu.make_async_copy(wo_ref, wof_ref.at[pl.ds(pl.multiple_of(s * OWN, OWN), OWN), :], lwo).start()

            @pl.when(t == 1)
            def _():
                w_across(3)

            @pl.when(t >= 2)
            def _():
                for k in range(PARTS):
                    wo_across((t - 2) * PARTS + k)

        @pl.when(t > 0)
        def _():
            attend_other(t - 1)

        @pl.when(t < STEPS)
        def _():
            attend_own(t)

    for k in range(PARTS, KP):
        wo_share(k)
    mine = wof_ref.at[pl.ds(pl.multiple_of(s * OWN, OWN), OWN), :]
    pltpu.make_async_copy(wo_ref, mine, lwo).wait()
    theirs = wof_ref.at[pl.ds(pl.multiple_of((s + 1 - 2 * c) * OWN, OWN), OWN), :]
    remote(wo_ref, mine, swo_send, swo_recv, sib).wait_send()
    remote(theirs, theirs, swo_send, swo_recv, sib).wait_recv()
    for i in range(4):
        a_copy(c, i).wait_send()
    for j in range(STEPS):
        here = place(j, s * SHARD, SHARD)
        remote(here, here, sw_send.at[j], sw_recv.at[j], sib).wait_send()
        for core in range(2):
            for r in range(CUT):
                here = place(j, s * SHARD + y * HALF + r * PIECE, PIECE)
                remote(here, here, xw_send.at[j, core, r], xw_recv.at[j, c, r], across(core)).wait_send()
                here = place(j, (other + core) * SHARD + y * HALF + r * PIECE, PIECE)
                remote(here, here, yw_send.at[j, core, r], yw_recv.at[j, core, r], twin).wait_send()

        @pl.when(chip == 0)
        def _():
            for copy in kv_copies(j):
                copy.wait_send()

        for i in range(2):
            seen_local(j, 2 * c + i).wait()
            seen_remote(j, 2 * (1 - c) + i).wait_send()
            here = seen_ref.at[pl.ds(i * BQ, BQ), pl.ds(pl.multiple_of((2 * j + 1 - c) * QC, QC), QC)]
            remote(here, here, so_send.at[j, 2 * c + i], so_recv.at[j, 2 * c + i], sib).wait_recv()
    for k in range(KP):
        for core in range(2):
            mine = wof_ref.at[wo_rows(s, 2 * y + core, k), :]
            remote(mine, mine, wx_send.at[k, core], wx_recv.at[k, c], across(core)).wait_send()
            here = wof_ref.at[wo_rows(other + core, 2 * y + c, k), :]
            remote(here, here, wy_send.at[k, core], wy_recv.at[k, core], twin).wait_send()
            remote(here, here, wsx_send.at[k, core], wsx_recv.at[k, core], sib).wait_send()
            here = wof_ref.at[wo_rows(other + core, 2 * (1 - y) + c, k), :]
            remote(here, here, wsy_send.at[k, core], wsy_recv.at[k, core], sib).wait_send()
            here = wof_ref.at[wo_rows(other + core, 2 * y + 1 - c, k), :]
            remote(here, here, wsx_send.at[k, core], wsx_recv.at[k, core], sib).wait_recv()
            here = wof_ref.at[wo_rows(other + core, 2 * (1 - y) + 1 - c, k), :]
            remote(here, here, wsy_send.at[k, core], wsy_recv.at[k, core], sib).wait_recv()


def _gather_and_attend(x, gain, freq, wq, wk, wv, wo):
    dma = lambda *shape: pltpu.SemaphoreType.DMA(shape) if shape else pltpu.SemaphoreType.DMA
    hbm, vmem = pl.BlockSpec(memory_space=pl.ANY), pl.BlockSpec(memory_space=pltpu.VMEM)
    bf16, f32 = jnp.bfloat16, jnp.float32
    return pl.pallas_call(
        _kernel,
        out_shape=[jax.ShapeDtypeStruct((OWN, 4 * OWN), bf16), jax.ShapeDtypeStruct((4 * OWN, D), bf16)],
        in_specs=[hbm, vmem, vmem, hbm, hbm, hbm, hbm],
        out_specs=[hbm, hbm],
        scratch_shapes=[
            pltpu.VMEM((CHIP, D), bf16), pltpu.VMEM((STEPS, D, WC), bf16), pltpu.VMEM((STEPS, 2, CHIP, HEAD), bf16),
            pltpu.VMEM((STEPS, 2, VR, CHIP), bf16), pltpu.VMEM((2, G, CHIP, HEAD), bf16), pltpu.VMEM((STEPS, CHIP // BQ, BQ, QC), bf16),
            pltpu.VMEM((CHIP, HEAD), f32), pltpu.VMEM((CHIP, HEAD), f32), pltpu.VMEM((CHIP // BQ, 1, COLS), f32), pltpu.VMEM((CHIP // BQ, VR, COLS), f32),
            dma(4), dma(4), dma(4), dma(4), dma(4), dma(4), dma(4, 2, CUT), dma(4, 2, CUT), dma(4, 2, CUT), dma(4, 2, CUT), dma(4, 2), dma(4, 2),
            dma(4, 4), dma(4, 4), dma(4, 4), dma(), dma(), dma(), dma(KP, 2), dma(KP, 2), dma(KP, 2), dma(KP, 2),
            dma(KP, 2), dma(KP, 2), dma(KP, 2), dma(KP, 2),
        ],
        compiler_params=pltpu.CompilerParams(collective_id=0, has_side_effects=True, vmem_limit_bytes=63 * 2**20),
        cost_estimate=pl.CostEstimate(flops=120 * 10**9, transcendentals=10**8, bytes_accessed=100 * 2**20),
    )(x, gain, freq, wq, wk, wv, wo)


def solution(mesh):
    def step(x, gain, wq, wk, wv, wo):
        half = HEAD // 2
        freq = THETA ** (-jnp.arange(half, dtype=jnp.float32) / half)
        freq = jnp.concatenate([freq, freq])[None]
        seen, whole = _gather_and_attend(x, gain[None], freq, wq, wk, wv, wo)
        y = jnp.dot(seen, whole, preferred_element_type=jnp.float32)
        return (x.astype(jnp.float32) + y).astype(jnp.bfloat16)

    tokens, rows = P(("dp", "sp"), None), P("sp", None)
    return jax.shard_map(
        step,
        mesh=mesh,
        in_specs=(tokens, P(None), rows, rows, rows, rows),
        out_specs=tokens,
        check_vma=False,
    )
```

```python
import functools

import jax
import jax.numpy as jnp
from jax import lax
from jax.experimental import pallas as pl
from jax.experimental.pallas import tpu as pltpu
from jax.sharding import PartitionSpec as P

HEAD = 128
THETA = 10000
NEG = -1e30
HIDDEN = 2 * NEG
LOG2E = 1.4426950408889634
D = 2560
OWN = 1024
CHIP = 2 * OWN
STEPS = 4
G = 4
QC = G * HEAD
WC = QC + 2 * HEAD
SHARD = D // 4
HALF = SHARD // 2
CUT = 2
PIECE = HALF // CUT
BQ = 512
BK = 512
COLS = G * BQ
SQ = 256
VR = HEAD + 16
NC = 256
KP = D // NC
PARTS = KP // 2
MESH = pl.DeviceIdType.MESH


def _dot(a, b, ca, cb):
    return lax.dot_general(a, b, (((ca,), (cb,)), ((), ())), preferred_element_type=jnp.float32)


def _kernel(x_ref, gain_ref, freq_ref, wq_ref, wk_ref, wv_ref, wo_ref, y_ref, wof_ref,
            a_s, w_s, k_s, v_s, q_s, st_s, seen_s, y_s, cos_s, sin_s, top_s, mix_s,
            lx, a_send, a_recv, lw, sw_send, sw_recv, xw_send, xw_recv, yw_send, yw_recv, kv_send, kv_recv,
            so_send, so_recv, tl, tx, ty, swo_send, swo_recv, wx_send, wx_recv, wy_send, wy_recv,
            wsx_send, wsx_recv, wsy_send, wsy_recv):
    y, s = lax.axis_index("dp"), lax.axis_index("sp")
    chip, c = lax.div(s, 2), lax.rem(s, 2)
    other = 2 * (1 - chip)
    sib = (y, s + 1 - 2 * c)
    across = lambda core: (y, other + core)
    twin = (1 - y, s)
    scale = HEAD**-0.5
    e = scale * LOG2E

    def remote(src, dst, send, recv, device):
        return pltpu.make_async_remote_copy(src_ref=src, dst_ref=dst, send_sem=send, recv_sem=recv, device_id=device, device_id_type=MESH)

    barrier = pltpu.get_barrier_semaphore()
    for device in (sib, across(0), across(1), twin):
        pl.semaphore_signal(barrier, inc=1, device_id=device, device_id_type=MESH)
    pl.semaphore_wait(barrier, 4)

    def pieces(core, j, row, n):
        h = 2 * j + core
        rows = pl.ds(row, n)
        return ((wq_ref.at[rows, pl.ds(pl.multiple_of(h * QC, QC), QC)], pl.ds(0, QC)),
                (wk_ref.at[rows, pl.ds(pl.multiple_of(h * HEAD, HEAD), HEAD)], pl.ds(QC, HEAD)),
                (wv_ref.at[rows, pl.ds(pl.multiple_of(h * HEAD, HEAD), HEAD)], pl.ds(QC + HEAD, HEAD)))

    def place(j, row, n):
        return w_s.at[j, pl.ds(pl.multiple_of(row, 32), n), :]

    def w_local(j):
        for src, cols in pieces(c, j, 0, SHARD):
            pltpu.make_async_copy(src, w_s.at[j, pl.ds(pl.multiple_of(s * SHARD, HALF), SHARD), cols], lw.at[j]).start()

    def w_sib(j):
        for src, cols in pieces(1 - c, j, 0, SHARD):
            remote(src, w_s.at[j, pl.ds(pl.multiple_of(s * SHARD, HALF), SHARD), cols], sw_send.at[j], sw_recv.at[j], sib).start()

    def w_across(j):
        for r in range(CUT):
            for core in range(2):
                row = pl.multiple_of(y * HALF + r * PIECE, 32)
                for src, cols in pieces(core, j, row, PIECE):
                    remote(src, w_s.at[j, pl.ds(pl.multiple_of(s * SHARD + y * HALF + r * PIECE, 32), PIECE), cols],
                           xw_send.at[j, core, r], xw_recv.at[j, c, r], across(core)).start()

    def w_forward(j, r):
        for core in range(2):
            here = place(j, (other + core) * SHARD + y * HALF + r * PIECE, PIECE)
            remote(here, here, xw_send.at[j, core, r], xw_recv.at[j, core, r], across(core)).wait_recv()
            remote(here, here, yw_send.at[j, core, r], yw_recv.at[j, core, r], twin).start()

    def w_wait(j):
        here = place(j, s * SHARD, SHARD)
        pltpu.make_async_copy(here, here, lw.at[j]).wait()
        here = place(j, (s + 1 - 2 * c) * SHARD, SHARD)
        remote(here, here, sw_send.at[j], sw_recv.at[j], sib).wait_recv()
        for core in range(2):
            for r in range(CUT):
                here = place(j, (other + core) * SHARD + (1 - y) * HALF + r * PIECE, PIECE)
                remote(here, here, yw_send.at[j, core, r], yw_recv.at[j, core, r], twin).wait_recv()

    def wo_place(owner, quarter, n):
        return wof_ref.at[pl.ds(pl.multiple_of(owner * OWN + quarter * 256, 256), 256), pl.ds(pl.multiple_of(n * NC, NC), NC)]

    def wo_across(n):
        for core in range(2):
            src = wo_ref.at[pl.ds(pl.multiple_of((2 * y + core) * 256, 256), 256), pl.ds(pl.multiple_of(n * NC, NC), NC)]
            remote(src, wo_place(s, 2 * y + core, n), wx_send.at[n, core], wx_recv.at[n, c], across(core)).start()

    def wo_forward(n):
        for core in range(2):
            here = wo_place(other + core, 2 * y + c, n)
            remote(here, here, wx_send.at[n, core], wx_recv.at[n, core], across(core)).wait_recv()
            remote(here, here, wy_send.at[n, core], wy_recv.at[n, core], twin).start()
            remote(here, here, wsx_send.at[n, core], wsx_recv.at[n, core], sib).start()

    def wo_share(n):
        for core in range(2):
            here = wo_place(other + core, 2 * (1 - y) + c, n)
            remote(here, here, wy_send.at[n, core], wy_recv.at[n, core], twin).wait_recv()
            remote(here, here, wsy_send.at[n, core], wsy_recv.at[n, core], sib).start()

    def fetch(n):
        for core in range(2):
            here = wo_place(other + core, 2 * y + 1 - c, n)
            remote(here, here, wsx_send.at[n, core], wsx_recv.at[n, core], sib).wait_recv()
            here = wo_place(other + core, 2 * (1 - y) + 1 - c, n)
            remote(here, here, wsy_send.at[n, core], wsy_recv.at[n, core], sib).wait_recv()
        slot = lax.rem(n, 2)
        cols = pl.ds(pl.multiple_of(n * NC, NC), NC)

        def take(src, core, half):
            dst = w_s.at[slot, pl.ds(pl.multiple_of(core * OWN, OWN), OWN), pl.ds(pl.multiple_of(half * NC, NC), NC)]
            pltpu.make_async_copy(src, dst, tl.at[slot]).start()

        take(wo_ref.at[:, cols], c, chip)
        take(wof_ref.at[pl.ds(pl.multiple_of((s + 1 - 2 * c) * OWN, OWN), OWN), cols], 1 - c, chip)
        for core in range(2):
            take(wof_ref.at[pl.ds(pl.multiple_of((other + core) * OWN, OWN), OWN), cols], core, 1 - chip)
        pltpu.make_async_copy(x_ref.at[:, cols], w_s.at[slot, :OWN, 2 * NC :], tx.at[slot]).start()

    def y_copy(n):
        return pltpu.make_async_copy(y_s.at[lax.rem(n, 2)], y_ref.at[:, pl.ds(pl.multiple_of(n * NC, NC), NC)], ty.at[lax.rem(n, 2)])

    def finish(n):
        slot = lax.rem(n, 2)
        here = w_s.at[slot, : 2 * OWN, : 2 * NC]
        pltpu.make_async_copy(here, here, tl.at[slot]).wait()
        here = w_s.at[slot, :OWN, 2 * NC :]
        pltpu.make_async_copy(here, here, tx.at[slot]).wait()

        @pl.when(n >= 2)
        def _():
            y_copy(n - 2).wait()

        got = _dot(seen_s[:, : 2 * OWN], w_s[slot, : 2 * OWN, :NC], 1, 0) + _dot(seen_s[:, 2 * OWN :], w_s[slot, : 2 * OWN, NC : 2 * NC], 1, 0)
        y_s[slot] = (w_s[slot, :OWN, 2 * NC :].astype(jnp.float32) + got).astype(jnp.bfloat16)
        y_copy(n).start()

    w_across(0)
    w_local(0)
    w_sib(0)
    w_across(1)
    for i in range(4):
        rows = pl.ds(pl.multiple_of(c * OWN + i * 256, 256), 256)
        pltpu.make_async_copy(x_ref.at[pl.ds(i * 256, 256), :], a_s.at[rows, :], lx.at[i]).start()

    @pl.loop(0, CHIP // 256)
    def _(i):
        rows = pl.ds(pl.multiple_of(i * 256, 256), 256)
        spot = (chip * CHIP + i * 256 + lax.broadcasted_iota(jnp.int32, (256, HEAD), 0)).astype(jnp.float32)
        angle = spot * freq_ref[...]
        cos_s[rows, :] = jnp.cos(angle)
        left = lax.broadcasted_iota(jnp.int32, (256, HEAD), 1) < HEAD // 2
        sin = jnp.sin(angle)
        sin_s[rows, :] = jnp.where(left, -sin, sin)

    gain = gain_ref[...].astype(jnp.float32)

    def a_rows(core, i):
        return a_s.at[pl.ds(pl.multiple_of(core * OWN + i * 256, 256), 256), :]

    def a_copy(core, i):
        return remote(a_rows(core, i), a_rows(core, i), a_send.at[i], a_recv.at[i], sib)

    for i in range(4):
        pltpu.make_async_copy(x_ref.at[pl.ds(i * 256, 256), :], a_rows(c, i), lx.at[i]).wait()

        @pl.loop(0, 256 // 32)
        def _(r):
            rows = pl.ds(pl.multiple_of(c * OWN + i * 256 + r * 32, 32), 32)
            wide = a_s[rows, :].astype(jnp.float32)
            inverse = lax.rsqrt(jnp.mean(wide * wide, -1, keepdims=True) + 1e-6)
            a_s[rows, :] = (wide * inverse * gain).astype(jnp.bfloat16)

        if i:
            a_copy(c, i - 1).start()
    for j in range(1, STEPS):
        w_local(j)
    v_s[:, :, HEAD:, :] = jnp.ones((STEPS, 2, VR - HEAD, CHIP), jnp.bfloat16)
    a_copy(c, 3).start()
    for j in range(1, STEPS):
        w_sib(j)
    for r in range(CUT):
        w_forward(0, r)
    for i in range(4):
        a_copy(1 - c, i).wait_recv()
    w_forward(1, 0)

    def project(t):
        slot = lax.rem(t, 2)

        @pl.loop(0, CHIP // 512)
        def _(m):
            rows = pl.ds(pl.multiple_of(m * 512, 512), 512)
            got = _dot(a_s[rows, :], w_s[t], 1, 0)
            cos, sin = cos_s[rows, :], sin_s[rows, :]
            for g in range(G + 1):
                part = got[:, g * HEAD : (g + 1) * HEAD].astype(jnp.bfloat16).astype(jnp.float32)
                part = (part * cos + pltpu.roll(part, HEAD // 2, 1) * sin).astype(jnp.bfloat16)
                if g < G:
                    q_s[slot, g, rows, :] = part
                else:
                    k_s[t, chip, rows, :] = part
            v_s[t, chip, :HEAD, rows] = got[:, QC + HEAD :].T.astype(jnp.bfloat16)

    def kv_copies(t):
        k, v = k_s.at[t, 0], v_s.at[t, 0, :HEAD, :]
        device = (y, 2 * (1 - chip) + c)
        return remote(k, k, kv_send.at[t, 0], kv_recv.at[t, 0], device), remote(v, v, kv_send.at[t, 1], kv_recv.at[t, 1], device)

    def seen_place(half, j, core):
        return seen_s.at[pl.ds(pl.multiple_of(half * BQ, BQ), BQ), pl.ds(pl.multiple_of((2 * j + core) * QC, QC), QC)]

    def seen_send(j, half):
        return remote(st_s.at[lax.rem(j, 2), half], seen_place(half, j, c), so_send.at[j, half], so_recv.at[j, half], sib)

    def queries(iq):
        return pl.ds(pl.multiple_of(iq * BQ, BQ), BQ)

    def block(j, iq, half, at):
        here = pl.ds(pl.multiple_of(at * BK, BK), BK)
        keys = k_s[j, half, here, :]
        scores = [_dot(keys, q_s[lax.rem(j, 2), g, queries(iq), :], 1, 1) for g in range(G)]
        weights, keeps = [], []
        for g, sc in enumerate(scores):
            cols = slice(g * BQ, (g + 1) * BQ)
            old = top_s[iq, :, cols]
            top = jnp.maximum(old, sc.max(axis=0, keepdims=True))
            top_s[iq, :, cols] = top
            keeps.append(jnp.exp2((old - top) * e))
            weights.append(jnp.exp2((sc - top) * e).astype(jnp.bfloat16))
        values = v_s[j, half, :, here]
        for g, p in enumerate(weights):
            cols = slice(g * BQ, (g + 1) * BQ)
            mix_s[iq, :, cols] = mix_s[iq, :, cols] * keeps[g] + _dot(values, p, 1, 0)

    def diagonal(j, iq):
        here = pl.multiple_of(iq * BQ, BQ)
        strips = [(g, at) for g in range(G) for at in range(0, BQ, SQ)]
        scores = [_dot(k_s[j, chip, pl.ds(here, at + SQ), :],
                       q_s[lax.rem(j, 2), g, pl.ds(pl.multiple_of(here + at, SQ), SQ), :], 1, 1) for g, at in strips]
        weights = []
        for (g, at), sc in zip(strips, scores):
            cols = slice(g * BQ + at, g * BQ + at + SQ)
            ok = lax.broadcasted_iota(jnp.int32, sc.shape, 1) + at >= lax.broadcasted_iota(jnp.int32, sc.shape, 0)
            sc = jnp.where(ok, sc, HIDDEN)
            top = sc.max(axis=0, keepdims=True)
            top_s[iq, :, cols] = top
            weights.append(jnp.exp2((sc - top) * e).astype(jnp.bfloat16))
        for (g, at), p in zip(strips, weights):
            mix_s[iq, :, g * BQ + at : g * BQ + at + SQ] = _dot(v_s[j, chip, :, pl.ds(here, at + SQ)], p, 1, 0)

    def attend_own(j):
        @pl.loop(0, CHIP // BQ)
        def _(iq):
            diagonal(j, iq)

            @pl.loop(0, iq)
            def _(i):
                block(j, iq, chip, i)

    def attend_other(j):
        @pl.when(chip == 1)
        def _():
            for copy in kv_copies(j):
                copy.wait_recv()

        @pl.loop(0, CHIP // BQ)
        def _(iq):
            @pl.when((j < 2) & (iq >= CHIP // BQ - CUT))
            def _():
                w_forward(j + 2, iq - (CHIP // BQ - CUT))

            @pl.when(j >= 2)
            def _():
                wo_forward((j - 2) * PARTS + iq)

            @pl.when(j == 3)
            def _():
                wo_share(iq)

            @pl.loop(0, chip * (CHIP // BK))
            def _(i):
                block(j, iq, 0, i)

            outs = []
            for g in range(G):
                cols = slice(g * BQ, (g + 1) * BQ)
                total = mix_s[iq, HEAD : HEAD + 1, cols]
                outs.append((mix_s[iq, :HEAD, cols] * (1 / total)).T.astype(jnp.bfloat16))
            half = lax.rem(iq, 2)

            @pl.when(lax.div(iq, 2) == c)
            def _():
                for g, out in enumerate(outs):
                    seen_s[pl.ds(pl.multiple_of(half * BQ, BQ), BQ), pl.ds(pl.multiple_of((2 * j + c) * QC + g * HEAD, HEAD), HEAD)] = out

            @pl.when(lax.div(iq, 2) != c)
            def _():
                @pl.when(j >= 2)
                def _():
                    seen_send(j - 2, half).wait_send()

                for g, out in enumerate(outs):
                    st_s[lax.rem(j, 2), half, :, g * HEAD : (g + 1) * HEAD] = out
                seen_send(j, half).start()

        @pl.when(j >= 2)
        def _():
            wo_forward((j - 2) * PARTS + PARTS - 1)

    @pl.loop(0, STEPS + 1)
    def _(t):
        @pl.when(t < STEPS)
        def _():
            w_wait(t)
            project(t)

            @pl.when(chip == 0)
            def _():
                for copy in kv_copies(t):
                    copy.start()

            @pl.when(t == 0)
            def _():
                w_across(2)
                w_forward(1, 1)
                remote(wo_ref, wof_ref.at[pl.ds(pl.multiple_of(s * OWN, OWN), OWN), :], swo_send, swo_recv, sib).start()

            @pl.when(t == 1)
            def _():
                w_across(3)

            @pl.when(t >= 2)
            def _():
                for k in range(PARTS):
                    wo_across((t - 2) * PARTS + k)

        @pl.when(t > 0)
        def _():
            attend_other(t - 1)

        @pl.when(t < STEPS)
        def _():
            attend_own(t)

    for j in range(STEPS):
        for core in range(2):
            for r in range(CUT):
                here = place(j, (other + core) * SHARD + y * HALF + r * PIECE, PIECE)
                remote(here, here, yw_send.at[j, core, r], yw_recv.at[j, core, r], twin).wait_send()
    theirs = wof_ref.at[pl.ds(pl.multiple_of((s + 1 - 2 * c) * OWN, OWN), OWN), :]
    remote(theirs, theirs, swo_send, swo_recv, sib).wait_recv()
    fetch(0)
    for j in range(STEPS):
        for half in range(2):
            here = seen_place(half, j, 1 - c)
            remote(here, here, so_send.at[j, half], so_recv.at[j, half], sib).wait_recv()

    @pl.loop(0, KP)
    def _(n):
        @pl.when((n + 1 >= PARTS - 1) & (n + 1 < KP))
        def _():
            wo_share(n + 1)

        @pl.when(n + 1 < KP)
        def _():
            fetch(n + 1)

        finish(n)

    for n in range(KP - 2, KP):
        y_copy(n).wait()
    mine = wof_ref.at[pl.ds(pl.multiple_of(s * OWN, OWN), OWN), :]
    remote(wo_ref, mine, swo_send, swo_recv, sib).wait_send()
    for i in range(4):
        a_copy(c, i).wait_send()
    for j in range(STEPS):
        here = place(j, s * SHARD, SHARD)
        remote(here, here, sw_send.at[j], sw_recv.at[j], sib).wait_send()
        for core in range(2):
            for r in range(CUT):
                here = place(j, s * SHARD + y * HALF + r * PIECE, PIECE)
                remote(here, here, xw_send.at[j, core, r], xw_recv.at[j, c, r], across(core)).wait_send()

        @pl.when(chip == 0)
        def _():
            for copy in kv_copies(j):
                copy.wait_send()

        if j >= 2:
            for half in range(2):
                seen_send(j, half).wait_send()
    for n in range(KP):
        for core in range(2):
            mine = wo_place(s, 2 * y + core, n)
            remote(mine, mine, wx_send.at[n, core], wx_recv.at[n, c], across(core)).wait_send()
            here = wo_place(other + core, 2 * y + c, n)
            remote(here, here, wy_send.at[n, core], wy_recv.at[n, core], twin).wait_send()
            remote(here, here, wsx_send.at[n, core], wsx_recv.at[n, core], sib).wait_send()
            here = wo_place(other + core, 2 * (1 - y) + c, n)
            remote(here, here, wsy_send.at[n, core], wsy_recv.at[n, core], sib).wait_send()


def _layer(x, gain, freq, wq, wk, wv, wo):
    dma = lambda *shape: pltpu.SemaphoreType.DMA(shape) if shape else pltpu.SemaphoreType.DMA
    hbm, vmem = pl.BlockSpec(memory_space=pl.ANY), pl.BlockSpec(memory_space=pltpu.VMEM)
    bf16, f32 = jnp.bfloat16, jnp.float32
    return pl.pallas_call(
        _kernel,
        out_shape=[jax.ShapeDtypeStruct((OWN, D), bf16), jax.ShapeDtypeStruct((4 * OWN, D), bf16)],
        in_specs=[hbm, vmem, vmem, hbm, hbm, hbm, hbm],
        out_specs=[hbm, hbm],
        scratch_shapes=[
            pltpu.VMEM((CHIP, D), bf16), pltpu.VMEM((STEPS, D, WC), bf16), pltpu.VMEM((STEPS, 2, CHIP, HEAD), bf16),
            pltpu.VMEM((STEPS, 2, VR, CHIP), bf16), pltpu.VMEM((2, G, CHIP, HEAD), bf16), pltpu.VMEM((2, 2, BQ, QC), bf16),
            pltpu.VMEM((OWN, 4 * OWN), bf16), pltpu.VMEM((2, OWN, NC), bf16),
            pltpu.VMEM((CHIP, HEAD), f32), pltpu.VMEM((CHIP, HEAD), f32), pltpu.VMEM((CHIP // BQ, 1, COLS), f32), pltpu.VMEM((CHIP // BQ, VR, COLS), f32),
            dma(4), dma(4), dma(4), dma(4), dma(4), dma(4), dma(4, 2, CUT), dma(4, 2, CUT), dma(4, 2, CUT), dma(4, 2, CUT), dma(4, 2), dma(4, 2),
            dma(4, 2), dma(4, 2), dma(2), dma(2), dma(2), dma(), dma(), dma(KP, 2), dma(KP, 2), dma(KP, 2), dma(KP, 2),
            dma(KP, 2), dma(KP, 2), dma(KP, 2), dma(KP, 2),
        ],
        compiler_params=pltpu.CompilerParams(collective_id=0, has_side_effects=True, vmem_limit_bytes=63 * 2**20),
        cost_estimate=pl.CostEstimate(flops=120 * 10**9, transcendentals=10**8, bytes_accessed=100 * 2**20),
    )(x, gain, freq, wq, wk, wv, wo)


def solution(mesh):
    def step(x, gain, wq, wk, wv, wo):
        half = HEAD // 2
        freq = THETA ** (-jnp.arange(half, dtype=jnp.float32) / half)
        freq = jnp.concatenate([freq, freq])[None]
        return _layer(x, gain[None], freq, wq, wk, wv, wo)[0]

    tokens, rows = P(("dp", "sp"), None), P("sp", None)
    return jax.shard_map(
        step,
        mesh=mesh,
        in_specs=(tokens, P(None), rows, rows, rows, rows),
        out_specs=tokens,
        check_vma=False,
    )
```

```python
import functools

import jax
import jax.numpy as jnp
import numpy as np
from jax import lax
from jax.experimental import pallas as pl
from jax.experimental.pallas import tpu as pltpu
from jax.sharding import PartitionSpec as P

HEAD = 128
THETA = 10000
NEG = -1e30
HIDDEN = 2 * NEG
LOG2E = 1.4426950408889634
D = 2560
OWN = 1024
CHIP = 2 * OWN
STEPS = 4
G = 4
QC = G * HEAD
WC = QC + 2 * HEAD
SHARD = D // 4
HALF = SHARD // 2
CUT = 2
PIECE = HALF // CUT
BQ = 512
BK = 512
COLS = G * BQ
SQ = 256
VR = HEAD + 16
NC = 256
KP = D // NC
PARTS = KP // 2
FORWARD = ((9, 0), (10, 1), (11, 2), (11, 3), (12, 4), (14, 5), (15, 6))
MESH = pl.DeviceIdType.MESH


def _dot(a, b, ca, cb):
    return lax.dot_general(a, b, (((ca,), (cb,)), ((), ())), preferred_element_type=jnp.float32)


def _kernel(x_ref, gain_ref, freq_ref, wq_ref, wk_ref, wv_ref, wo_ref, y_ref, wof_ref,
            a_s, w_s, k_s, v_s, q_s, st_s, seen_s, y_s, cos_s, sin_s, top_s, mix_s,
            lx, a_send, a_recv, lw, sw_send, sw_recv, xw_send, xw_recv, yw_send, yw_recv, kv_send, kv_recv,
            so_send, so_recv, tl, tx, ty, swo_send, swo_recv, wx_send, wx_recv, wy_send, wy_recv,
            wsx_send, wsx_recv, wsy_send, wsy_recv):
    y, s = lax.axis_index("dp"), lax.axis_index("sp")
    chip, c = lax.div(s, 2), lax.rem(s, 2)
    other = 2 * (1 - chip)
    sib = (y, s + 1 - 2 * c)
    across = lambda core: (y, other + core)
    twin = (1 - y, s)
    scale = HEAD**-0.5
    e = scale * LOG2E

    def remote(src, dst, send, recv, device):
        return pltpu.make_async_remote_copy(src_ref=src, dst_ref=dst, send_sem=send, recv_sem=recv, device_id=device, device_id_type=MESH)

    barrier = pltpu.get_barrier_semaphore()
    for device in (sib, across(0), across(1), twin):
        pl.semaphore_signal(barrier, inc=1, device_id=device, device_id_type=MESH)
    pl.semaphore_wait(barrier, 4)

    def pieces(core, j, row, n):
        h = 2 * j + core
        rows = pl.ds(row, n)
        return ((wq_ref.at[rows, pl.ds(pl.multiple_of(h * QC, QC), QC)], pl.ds(0, QC)),
                (wk_ref.at[rows, pl.ds(pl.multiple_of(h * HEAD, HEAD), HEAD)], pl.ds(QC, HEAD)),
                (wv_ref.at[rows, pl.ds(pl.multiple_of(h * HEAD, HEAD), HEAD)], pl.ds(QC + HEAD, HEAD)))

    def place(j, row, n):
        return w_s.at[j, pl.ds(pl.multiple_of(row, 32), n), :]

    def w_local(j):
        for src, cols in pieces(c, j, 0, SHARD):
            pltpu.make_async_copy(src, w_s.at[j, pl.ds(pl.multiple_of(s * SHARD, HALF), SHARD), cols], lw.at[j]).start()

    def w_sib(j):
        for src, cols in pieces(1 - c, j, 0, SHARD):
            remote(src, w_s.at[j, pl.ds(pl.multiple_of(s * SHARD, HALF), SHARD), cols], sw_send.at[j], sw_recv.at[j], sib).start()

    def w_across(j):
        for r in range(CUT):
            for core in range(2):
                row = pl.multiple_of(y * HALF + r * PIECE, 32)
                for src, cols in pieces(core, j, row, PIECE):
                    remote(src, w_s.at[j, pl.ds(pl.multiple_of(s * SHARD + y * HALF + r * PIECE, 32), PIECE), cols],
                           xw_send.at[j, core, r], xw_recv.at[j, c, r], across(core)).start()

    def w_forward(j, r):
        for core in range(2):
            here = place(j, (other + core) * SHARD + y * HALF + r * PIECE, PIECE)
            remote(here, here, xw_send.at[j, core, r], xw_recv.at[j, core, r], across(core)).wait_recv()
            remote(here, here, yw_send.at[j, core, r], yw_recv.at[j, core, r], twin).start()

    def w_wait(j):
        here = place(j, s * SHARD, SHARD)
        pltpu.make_async_copy(here, here, lw.at[j]).wait()
        here = place(j, (s + 1 - 2 * c) * SHARD, SHARD)
        remote(here, here, sw_send.at[j], sw_recv.at[j], sib).wait_recv()
        for core in range(2):
            for r in range(CUT):
                here = place(j, (other + core) * SHARD + (1 - y) * HALF + r * PIECE, PIECE)
                remote(here, here, yw_send.at[j, core, r], yw_recv.at[j, core, r], twin).wait_recv()

    def wo_place(owner, quarter, n):
        return wof_ref.at[pl.ds(pl.multiple_of(owner * OWN + quarter * 256, 256), 256), pl.ds(pl.multiple_of(n * NC, NC), NC)]

    def wo_across(n):
        for core in range(2):
            src = wo_ref.at[pl.ds(pl.multiple_of((2 * y + core) * 256, 256), 256), pl.ds(pl.multiple_of(n * NC, NC), NC)]
            remote(src, wo_place(s, 2 * y + core, n), wx_send.at[n, core], wx_recv.at[n, c], across(core)).start()

    def wo_forward(n):
        for core in range(2):
            here = wo_place(other + core, 2 * y + c, n)
            remote(here, here, wx_send.at[n, core], wx_recv.at[n, core], across(core)).wait_recv()
            remote(here, here, wy_send.at[n, core], wy_recv.at[n, core], twin).start()
            remote(here, here, wsx_send.at[n, core], wsx_recv.at[n, core], sib).start()

    def wo_share(n):
        for core in range(2):
            here = wo_place(other + core, 2 * (1 - y) + c, n)
            remote(here, here, wy_send.at[n, core], wy_recv.at[n, core], twin).wait_recv()
            remote(here, here, wsy_send.at[n, core], wsy_recv.at[n, core], sib).start()

    def fetch(n):
        for core in range(2):
            here = wo_place(other + core, 2 * y + 1 - c, n)
            remote(here, here, wsx_send.at[n, core], wsx_recv.at[n, core], sib).wait_recv()
            here = wo_place(other + core, 2 * (1 - y) + 1 - c, n)
            remote(here, here, wsy_send.at[n, core], wsy_recv.at[n, core], sib).wait_recv()
        slot = lax.rem(n, 2)
        cols = pl.ds(pl.multiple_of(n * NC, NC), NC)

        def take(src, core, half):
            dst = w_s.at[slot, pl.ds(pl.multiple_of(core * OWN, OWN), OWN), pl.ds(pl.multiple_of(half * NC, NC), NC)]
            pltpu.make_async_copy(src, dst, tl.at[slot]).start()

        take(wo_ref.at[:, cols], c, chip)
        take(wof_ref.at[pl.ds(pl.multiple_of((s + 1 - 2 * c) * OWN, OWN), OWN), cols], 1 - c, chip)
        for core in range(2):
            take(wof_ref.at[pl.ds(pl.multiple_of((other + core) * OWN, OWN), OWN), cols], core, 1 - chip)
        pltpu.make_async_copy(x_ref.at[:, cols], w_s.at[slot, :OWN, 2 * NC :], tx.at[slot]).start()

    def y_copy(n):
        return pltpu.make_async_copy(y_s.at[lax.rem(n, 2)], y_ref.at[:, pl.ds(pl.multiple_of(n * NC, NC), NC)], ty.at[lax.rem(n, 2)])

    def finish(n):
        slot = lax.rem(n, 2)
        here = w_s.at[slot, : 2 * OWN, : 2 * NC]
        pltpu.make_async_copy(here, here, tl.at[slot]).wait()
        here = w_s.at[slot, :OWN, 2 * NC :]
        pltpu.make_async_copy(here, here, tx.at[slot]).wait()

        @pl.when(n >= 2)
        def _():
            y_copy(n - 2).wait()

        got = _dot(seen_s[:, : 2 * OWN], w_s[slot, : 2 * OWN, :NC], 1, 0) + _dot(seen_s[:, 2 * OWN :], w_s[slot, : 2 * OWN, NC : 2 * NC], 1, 0)
        y_s[slot] = (w_s[slot, :OWN, 2 * NC :].astype(jnp.float32) + got).astype(jnp.bfloat16)
        y_copy(n).start()

    w_across(0)
    w_local(0)
    w_sib(0)
    w_across(1)
    for i in range(4):
        rows = pl.ds(pl.multiple_of(c * OWN + i * 256, 256), 256)
        pltpu.make_async_copy(x_ref.at[pl.ds(i * 256, 256), :], a_s.at[rows, :], lx.at[i]).start()

    @pl.loop(0, CHIP // 256)
    def _(i):
        rows = pl.ds(pl.multiple_of(i * 256, 256), 256)
        spot = (chip * CHIP + i * 256 + lax.broadcasted_iota(jnp.int32, (256, HEAD), 0)).astype(jnp.float32)
        angle = spot * freq_ref[...]
        cos_s[rows, :] = jnp.cos(angle)
        left = lax.broadcasted_iota(jnp.int32, (256, HEAD), 1) < HEAD // 2
        sin = jnp.sin(angle)
        sin_s[rows, :] = jnp.where(left, -sin, sin)

    gain = gain_ref[...].astype(jnp.float32)

    def a_rows(core, i):
        return a_s.at[pl.ds(pl.multiple_of(core * OWN + i * 256, 256), 256), :]

    def a_copy(core, i):
        return remote(a_rows(core, i), a_rows(core, i), a_send.at[i], a_recv.at[i], sib)

    for i in range(4):
        pltpu.make_async_copy(x_ref.at[pl.ds(i * 256, 256), :], a_rows(c, i), lx.at[i]).wait()

        @pl.loop(0, 256 // 32)
        def _(r):
            rows = pl.ds(pl.multiple_of(c * OWN + i * 256 + r * 32, 32), 32)
            wide = a_s[rows, :].astype(jnp.float32)
            inverse = lax.rsqrt(jnp.mean(wide * wide, -1, keepdims=True) + 1e-6)
            a_s[rows, :] = (wide * inverse * gain).astype(jnp.bfloat16)

        if i:
            a_copy(c, i - 1).start()
    for j in range(1, STEPS):
        w_local(j)
    v_s[:, :, HEAD:, :] = jnp.ones((STEPS, 2, VR - HEAD, CHIP), jnp.bfloat16)
    a_copy(c, 3).start()
    for j in range(1, STEPS):
        w_sib(j)
    for r in range(CUT):
        w_forward(0, r)
    for i in range(4):
        a_copy(1 - c, i).wait_recv()
    w_forward(1, 0)

    def project(t):
        slot = lax.rem(t, 2)

        @pl.loop(0, CHIP // 512)
        def _(m):
            rows = pl.ds(pl.multiple_of(m * 512, 512), 512)
            got = _dot(a_s[rows, :], w_s[t], 1, 0)
            cos, sin = cos_s[rows, :], sin_s[rows, :]
            for g in range(G + 1):
                part = got[:, g * HEAD : (g + 1) * HEAD].astype(jnp.bfloat16).astype(jnp.float32)
                part = (part * cos + pltpu.roll(part, HEAD // 2, 1) * sin).astype(jnp.bfloat16)
                if g < G:
                    q_s[slot, g, rows, :] = part
                else:
                    k_s[t, chip, rows, :] = part
            v_s[t, chip, :HEAD, rows] = got[:, QC + HEAD :].T.astype(jnp.bfloat16)

    def kv_copies(t):
        k, v = k_s.at[t, 0], v_s.at[t, 0, :HEAD, :]
        device = (y, 2 * (1 - chip) + c)
        return remote(k, k, kv_send.at[t, 0], kv_recv.at[t, 0], device), remote(v, v, kv_send.at[t, 1], kv_recv.at[t, 1], device)

    def seen_place(half, j, core):
        return seen_s.at[pl.ds(pl.multiple_of(half * BQ, BQ), BQ), pl.ds(pl.multiple_of((2 * j + core) * QC, QC), QC)]

    def seen_send(j, half):
        return remote(st_s.at[lax.rem(j, 2), half], seen_place(half, j, c), so_send.at[j, half], so_recv.at[j, half], sib)

    def queries(iq):
        return pl.ds(pl.multiple_of(iq * BQ, BQ), BQ)

    def block(j, iq, half, at):
        here = pl.ds(pl.multiple_of(at * BK, BK), BK)
        keys = k_s[j, half, here, :]
        scores = [_dot(keys, q_s[lax.rem(j, 2), g, queries(iq), :], 1, 1) for g in range(G)]
        weights, keeps = [], []
        for g, sc in enumerate(scores):
            cols = slice(g * BQ, (g + 1) * BQ)
            old = top_s[iq, :, cols]
            top = jnp.maximum(old, sc.max(axis=0, keepdims=True))
            top_s[iq, :, cols] = top
            keeps.append(jnp.exp2((old - top) * e))
            weights.append(jnp.exp2((sc - top) * e).astype(jnp.bfloat16))
        values = v_s[j, half, :, here]
        for g, p in enumerate(weights):
            cols = slice(g * BQ, (g + 1) * BQ)
            mix_s[iq, :, cols] = mix_s[iq, :, cols] * keeps[g] + _dot(values, p, 1, 0)

    def diagonal(j, iq):
        here = pl.multiple_of(iq * BQ, BQ)
        strips = [(g, at) for g in range(G) for at in range(0, BQ, SQ)]
        scores = [_dot(k_s[j, chip, pl.ds(here, at + SQ), :],
                       q_s[lax.rem(j, 2), g, pl.ds(pl.multiple_of(here + at, SQ), SQ), :], 1, 1) for g, at in strips]
        weights = []
        for (g, at), sc in zip(strips, scores):
            cols = slice(g * BQ + at, g * BQ + at + SQ)
            ok = lax.broadcasted_iota(jnp.int32, sc.shape, 1) + at >= lax.broadcasted_iota(jnp.int32, sc.shape, 0)
            sc = jnp.where(ok, sc, HIDDEN)
            top = sc.max(axis=0, keepdims=True)
            top_s[iq, :, cols] = top
            weights.append(jnp.exp2((sc - top) * e).astype(jnp.bfloat16))
        for (g, at), p in zip(strips, weights):
            mix_s[iq, :, g * BQ + at : g * BQ + at + SQ] = _dot(v_s[j, chip, :, pl.ds(here, at + SQ)], p, 1, 0)

    def attend_own(j):
        @pl.loop(0, CHIP // BQ)
        def _(iq):
            diagonal(j, iq)

            @pl.loop(0, iq)
            def _(i):
                block(j, iq, chip, i)

    def attend_other(j):
        @pl.when(chip == 1)
        def _():
            for copy in kv_copies(j):
                copy.wait_recv()

        @pl.loop(0, CHIP // BQ)
        def _(iq):
            @pl.when((j < 2) & (iq >= CHIP // BQ - CUT))
            def _():
                w_forward(j + 2, iq - (CHIP // BQ - CUT))

            for at, n in FORWARD:
                @pl.when((j == at // 4) & (iq == at % 4))
                def _():
                    wo_forward(n)

            @pl.when(j == 3)
            def _():
                wo_share(iq)

            @pl.loop(0, chip * (CHIP // BK))
            def _(i):
                block(j, iq, 0, i)

            outs = []
            for g in range(G):
                cols = slice(g * BQ, (g + 1) * BQ)
                total = mix_s[iq, HEAD : HEAD + 1, cols]
                outs.append((mix_s[iq, :HEAD, cols] * (1 / total)).T.astype(jnp.bfloat16))
            half = lax.rem(iq, 2)

            @pl.when(lax.div(iq, 2) == c)
            def _():
                for g, out in enumerate(outs):
                    seen_s[pl.ds(pl.multiple_of(half * BQ, BQ), BQ), pl.ds(pl.multiple_of((2 * j + c) * QC + g * HEAD, HEAD), HEAD)] = out

            @pl.when(lax.div(iq, 2) != c)
            def _():
                @pl.when(j >= 2)
                def _():
                    seen_send(j - 2, half).wait_send()

                for g, out in enumerate(outs):
                    st_s[lax.rem(j, 2), half, :, g * HEAD : (g + 1) * HEAD] = out
                seen_send(j, half).start()

    @pl.loop(0, STEPS + 1)
    def _(t):
        @pl.when(t < STEPS)
        def _():
            w_wait(t)
            project(t)

            @pl.when(chip == 0)
            def _():
                for copy in kv_copies(t):
                    copy.start()

            @pl.when(t == 0)
            def _():
                w_across(2)
                w_forward(1, 1)
                remote(wo_ref, wof_ref.at[pl.ds(pl.multiple_of(s * OWN, OWN), OWN), :], swo_send, swo_recv, sib).start()

            @pl.when(t == 1)
            def _():
                w_across(3)

            @pl.when(t >= 2)
            def _():
                for k in range(PARTS):
                    wo_across((t - 2) * PARTS + k)

        @pl.when(t > 0)
        def _():
            attend_other(t - 1)

        @pl.when(t < STEPS)
        def _():
            attend_own(t)

    for j in range(STEPS):
        for core in range(2):
            for r in range(CUT):
                here = place(j, (other + core) * SHARD + y * HALF + r * PIECE, PIECE)
                remote(here, here, yw_send.at[j, core, r], yw_recv.at[j, core, r], twin).wait_send()
    theirs = wof_ref.at[pl.ds(pl.multiple_of((s + 1 - 2 * c) * OWN, OWN), OWN), :]
    remote(theirs, theirs, swo_send, swo_recv, sib).wait_recv()
    wo_forward(7)
    fetch(0)
    wo_forward(8)
    wo_share(4)
    for j in range(STEPS):
        for half in range(2):
            here = seen_place(half, j, 1 - c)
            remote(here, here, so_send.at[j, half], so_recv.at[j, half], sib).wait_recv()

    @pl.loop(0, KP)
    def _(n):
        @pl.when(n == 2)
        def _():
            wo_forward(9)

        @pl.when((n >= 3) & (n + 2 < KP))
        def _():
            wo_share(n + 2)

        @pl.when(n + 1 < KP)
        def _():
            fetch(n + 1)

        finish(n)

    for n in range(KP - 2, KP):
        y_copy(n).wait()
    mine = wof_ref.at[pl.ds(pl.multiple_of(s * OWN, OWN), OWN), :]
    remote(wo_ref, mine, swo_send, swo_recv, sib).wait_send()
    for i in range(4):
        a_copy(c, i).wait_send()
    for j in range(STEPS):
        here = place(j, s * SHARD, SHARD)
        remote(here, here, sw_send.at[j], sw_recv.at[j], sib).wait_send()
        for core in range(2):
            for r in range(CUT):
                here = place(j, s * SHARD + y * HALF + r * PIECE, PIECE)
                remote(here, here, xw_send.at[j, core, r], xw_recv.at[j, c, r], across(core)).wait_send()

        @pl.when(chip == 0)
        def _():
            for copy in kv_copies(j):
                copy.wait_send()

        if j >= 2:
            for half in range(2):
                seen_send(j, half).wait_send()
    for n in range(KP):
        for core in range(2):
            mine = wo_place(s, 2 * y + core, n)
            remote(mine, mine, wx_send.at[n, core], wx_recv.at[n, c], across(core)).wait_send()
            here = wo_place(other + core, 2 * y + c, n)
            remote(here, here, wy_send.at[n, core], wy_recv.at[n, core], twin).wait_send()
            remote(here, here, wsx_send.at[n, core], wsx_recv.at[n, core], sib).wait_send()
            here = wo_place(other + core, 2 * (1 - y) + c, n)
            remote(here, here, wsy_send.at[n, core], wsy_recv.at[n, core], sib).wait_send()


def _layer(x, gain, freq, wq, wk, wv, wo):
    dma = lambda *shape: pltpu.SemaphoreType.DMA(shape) if shape else pltpu.SemaphoreType.DMA
    hbm, vmem = pl.BlockSpec(memory_space=pl.ANY), pl.BlockSpec(memory_space=pltpu.VMEM)
    bf16, f32 = jnp.bfloat16, jnp.float32
    return pl.pallas_call(
        _kernel,
        out_shape=[jax.ShapeDtypeStruct((OWN, D), bf16), jax.ShapeDtypeStruct((4 * OWN, D), bf16)],
        in_specs=[hbm, vmem, vmem, hbm, hbm, hbm, hbm],
        out_specs=[hbm, hbm],
        scratch_shapes=[
            pltpu.VMEM((CHIP, D), bf16), pltpu.VMEM((STEPS, D, WC), bf16), pltpu.VMEM((STEPS, 2, CHIP, HEAD), bf16),
            pltpu.VMEM((STEPS, 2, VR, CHIP), bf16), pltpu.VMEM((2, G, CHIP, HEAD), bf16), pltpu.VMEM((2, 2, BQ, QC), bf16),
            pltpu.VMEM((OWN, 4 * OWN), bf16), pltpu.VMEM((2, OWN, NC), bf16),
            pltpu.VMEM((CHIP, HEAD), f32), pltpu.VMEM((CHIP, HEAD), f32), pltpu.VMEM((CHIP // BQ, 1, COLS), f32), pltpu.VMEM((CHIP // BQ, VR, COLS), f32),
            dma(4), dma(4), dma(4), dma(4), dma(4), dma(4), dma(4, 2, CUT), dma(4, 2, CUT), dma(4, 2, CUT), dma(4, 2, CUT), dma(4, 2), dma(4, 2),
            dma(4, 2), dma(4, 2), dma(2), dma(2), dma(2), dma(), dma(), dma(KP, 2), dma(KP, 2), dma(KP, 2), dma(KP, 2),
            dma(KP, 2), dma(KP, 2), dma(KP, 2), dma(KP, 2),
        ],
        compiler_params=pltpu.CompilerParams(collective_id=0, has_side_effects=True, vmem_limit_bytes=63 * 2**20),
        cost_estimate=pl.CostEstimate(flops=120 * 10**9, transcendentals=10**8, bytes_accessed=100 * 2**20),
    )(x, gain, freq, wq, wk, wv, wo)


def solution(mesh):
    def step(x, gain, wq, wk, wv, wo):
        half = HEAD // 2
        freq = np.float32(THETA) ** (-np.arange(half, dtype=np.float32) / np.float32(half))
        freq = jnp.asarray(np.concatenate([freq, freq])[None], jnp.float32)
        return _layer(x, gain[None], freq, wq, wk, wv, wo)[0]

    tokens, rows = P(("dp", "sp"), None), P("sp", None)
    return jax.shard_map(
        step,
        mesh=mesh,
        in_specs=(tokens, P(None), rows, rows, rows, rows),
        out_specs=tokens,
        check_vma=False,
    )
```

```python
import functools

import jax
import jax.numpy as jnp
import numpy as np
from jax import lax
from jax.experimental import pallas as pl
from jax.experimental.pallas import tpu as pltpu
from jax.sharding import PartitionSpec as P

HEAD = 128
THETA = 10000
NEG = -1e30
HIDDEN = 2 * NEG
LOG2E = 1.4426950408889634
D = 2560
OWN = 1024
CHIP = 2 * OWN
STEPS = 4
G = 4
QC = G * HEAD
WC = QC + 2 * HEAD
SHARD = D // 4
HALF = SHARD // 2
CUT = 4
PIECE = HALF // CUT
BQ = 512
BK = 512
COLS = G * BQ
SQ = 256
VR = HEAD + 16
NC = 256
KP = D // NC
FORWARD = ((9, 0), (12, 3), (13, 4), (14, 5), (15, 6))
FORWARD_OWN = ((13, 1), (15, 2))
MESH = pl.DeviceIdType.MESH


def _dot(a, b, ca, cb):
    return lax.dot_general(a, b, (((ca,), (cb,)), ((), ())), preferred_element_type=jnp.float32)


def _kernel(x_ref, gain_ref, freq_ref, wq_ref, wk_ref, wv_ref, wo_ref, y_ref, wof_ref,
            a_s, w_s, k_s, v_s, q_s, st_s, seen_s, y_s, cos_s, sin_s, top_s, mix_s,
            lx, a_send, a_recv, lw, sw_send, sw_recv, xw_send, xw_recv, yw_send, yw_recv, kv_send, kv_recv,
            so_send, so_recv, tl, tx, ty, swo_send, swo_recv, wx_send, wx_recv, wy_send, wy_recv,
            wsx_send, wsx_recv, wsy_send, wsy_recv):
    y, s = lax.axis_index("dp"), lax.axis_index("sp")
    chip, c = lax.div(s, 2), lax.rem(s, 2)
    other = 2 * (1 - chip)
    sib = (y, s + 1 - 2 * c)
    across = lambda core: (y, other + core)
    twin = (1 - y, s)
    scale = HEAD**-0.5
    e = scale * LOG2E

    def remote(src, dst, send, recv, device):
        return pltpu.make_async_remote_copy(src_ref=src, dst_ref=dst, send_sem=send, recv_sem=recv, device_id=device, device_id_type=MESH)

    barrier = pltpu.get_barrier_semaphore()
    for device in (sib, across(0), across(1), twin):
        pl.semaphore_signal(barrier, inc=1, device_id=device, device_id_type=MESH)
    pl.semaphore_wait(barrier, 4)

    def pieces(core, j, row, n):
        h = 2 * j + core
        rows = pl.ds(row, n)
        return ((wq_ref.at[rows, pl.ds(pl.multiple_of(h * QC, QC), QC)], pl.ds(0, QC)),
                (wk_ref.at[rows, pl.ds(pl.multiple_of(h * HEAD, HEAD), HEAD)], pl.ds(QC, HEAD)),
                (wv_ref.at[rows, pl.ds(pl.multiple_of(h * HEAD, HEAD), HEAD)], pl.ds(QC + HEAD, HEAD)))

    def place(j, row, n):
        return w_s.at[j, pl.ds(pl.multiple_of(row, 16), n), :]

    def w_local(j):
        for src, cols in pieces(c, j, 0, SHARD):
            pltpu.make_async_copy(src, w_s.at[j, pl.ds(pl.multiple_of(s * SHARD, HALF), SHARD), cols], lw.at[j]).start()

    def w_sib(j):
        for src, cols in pieces(1 - c, j, 0, SHARD):
            remote(src, w_s.at[j, pl.ds(pl.multiple_of(s * SHARD, HALF), SHARD), cols], sw_send.at[j], sw_recv.at[j], sib).start()

    def w_across(j):
        for r in range(CUT):
            for core in range(2):
                row = pl.multiple_of(y * HALF + r * PIECE, 16)
                for src, cols in pieces(core, j, row, PIECE):
                    remote(src, w_s.at[j, pl.ds(pl.multiple_of(s * SHARD + y * HALF + r * PIECE, 16), PIECE), cols],
                           xw_send.at[j, core, r], xw_recv.at[j, c, r], across(core)).start()

    def w_forward(j, r):
        for core in range(2):
            here = place(j, (other + core) * SHARD + y * HALF + r * PIECE, PIECE)
            remote(here, here, xw_send.at[j, core, r], xw_recv.at[j, core, r], across(core)).wait_recv()
            remote(here, here, yw_send.at[j, core, r], yw_recv.at[j, core, r], twin).start()

    def w_wait(j):
        here = place(j, s * SHARD, SHARD)
        pltpu.make_async_copy(here, here, lw.at[j]).wait()
        here = place(j, (s + 1 - 2 * c) * SHARD, SHARD)
        remote(here, here, sw_send.at[j], sw_recv.at[j], sib).wait_recv()
        for core in range(2):
            for r in range(CUT):
                here = place(j, (other + core) * SHARD + (1 - y) * HALF + r * PIECE, PIECE)
                remote(here, here, yw_send.at[j, core, r], yw_recv.at[j, core, r], twin).wait_recv()

    def wo_place(owner, quarter, n):
        return wof_ref.at[pl.ds(pl.multiple_of(owner * OWN + quarter * 256, 256), 256), pl.ds(pl.multiple_of(n * NC, NC), NC)]

    def wo_across(n):
        for core in range(2):
            src = wo_ref.at[pl.ds(pl.multiple_of((2 * y + core) * 256, 256), 256), pl.ds(pl.multiple_of(n * NC, NC), NC)]
            remote(src, wo_place(s, 2 * y + core, n), wx_send.at[n, core], wx_recv.at[n, c], across(core)).start()

    def wo_forward(n):
        for core in range(2):
            here = wo_place(other + core, 2 * y + c, n)
            remote(here, here, wx_send.at[n, core], wx_recv.at[n, core], across(core)).wait_recv()
            remote(here, here, wy_send.at[n, core], wy_recv.at[n, core], twin).start()
            remote(here, here, wsx_send.at[n, core], wsx_recv.at[n, core], sib).start()

    def wo_share(n):
        for core in range(2):
            here = wo_place(other + core, 2 * (1 - y) + c, n)
            remote(here, here, wy_send.at[n, core], wy_recv.at[n, core], twin).wait_recv()
            remote(here, here, wsy_send.at[n, core], wsy_recv.at[n, core], sib).start()

    def fetch(n):
        for core in range(2):
            here = wo_place(other + core, 2 * y + 1 - c, n)
            remote(here, here, wsx_send.at[n, core], wsx_recv.at[n, core], sib).wait_recv()
            here = wo_place(other + core, 2 * (1 - y) + 1 - c, n)
            remote(here, here, wsy_send.at[n, core], wsy_recv.at[n, core], sib).wait_recv()
        slot = lax.rem(n, 2)
        cols = pl.ds(pl.multiple_of(n * NC, NC), NC)

        def take(src, core, half):
            dst = w_s.at[slot, pl.ds(pl.multiple_of(core * OWN, OWN), OWN), pl.ds(pl.multiple_of(half * NC, NC), NC)]
            pltpu.make_async_copy(src, dst, tl.at[slot]).start()

        take(wo_ref.at[:, cols], c, chip)
        take(wof_ref.at[pl.ds(pl.multiple_of((s + 1 - 2 * c) * OWN, OWN), OWN), cols], 1 - c, chip)
        for core in range(2):
            take(wof_ref.at[pl.ds(pl.multiple_of((other + core) * OWN, OWN), OWN), cols], core, 1 - chip)
        pltpu.make_async_copy(x_ref.at[:, cols], w_s.at[slot, :OWN, 2 * NC :], tx.at[slot]).start()

    def y_copy(n):
        return pltpu.make_async_copy(y_s.at[lax.rem(n, 2)], y_ref.at[:, pl.ds(pl.multiple_of(n * NC, NC), NC)], ty.at[lax.rem(n, 2)])

    def finish(n):
        slot = lax.rem(n, 2)
        here = w_s.at[slot, : 2 * OWN, : 2 * NC]
        pltpu.make_async_copy(here, here, tl.at[slot]).wait()
        here = w_s.at[slot, :OWN, 2 * NC :]
        pltpu.make_async_copy(here, here, tx.at[slot]).wait()

        @pl.when(n >= 2)
        def _():
            y_copy(n - 2).wait()

        got = _dot(seen_s[:, : 2 * OWN], w_s[slot, : 2 * OWN, :NC], 1, 0) + _dot(seen_s[:, 2 * OWN :], w_s[slot, : 2 * OWN, NC : 2 * NC], 1, 0)
        y_s[slot] = (w_s[slot, :OWN, 2 * NC :].astype(jnp.float32) + got).astype(jnp.bfloat16)
        y_copy(n).start()

    w_across(0)
    w_local(0)
    w_sib(0)
    w_across(1)
    for i in range(4):
        rows = pl.ds(pl.multiple_of(c * OWN + i * 256, 256), 256)
        pltpu.make_async_copy(x_ref.at[pl.ds(i * 256, 256), :], a_s.at[rows, :], lx.at[i]).start()

    @pl.loop(0, CHIP // 256)
    def _(i):
        rows = pl.ds(pl.multiple_of(i * 256, 256), 256)
        spot = (chip * CHIP + i * 256 + lax.broadcasted_iota(jnp.int32, (256, HEAD), 0)).astype(jnp.float32)
        angle = spot * freq_ref[...]
        cos_s[rows, :] = jnp.cos(angle)
        left = lax.broadcasted_iota(jnp.int32, (256, HEAD), 1) < HEAD // 2
        sin = jnp.sin(angle)
        sin_s[rows, :] = jnp.where(left, -sin, sin)

    w_forward(0, 0)
    gain = gain_ref[...].astype(jnp.float32)[None]

    def a_rows(core, i):
        return a_s.at[pl.ds(pl.multiple_of(core * OWN + i * 256, 256), 256), :]

    def a_copy(core, i):
        return remote(a_rows(core, i), a_rows(core, i), a_send.at[i], a_recv.at[i], sib)

    for i in range(4):
        pltpu.make_async_copy(x_ref.at[pl.ds(i * 256, 256), :], a_rows(c, i), lx.at[i]).wait()

        @pl.loop(0, 256 // 32)
        def _(r):
            rows = pl.ds(pl.multiple_of(c * OWN + i * 256 + r * 32, 32), 32)
            wide = a_s[rows, :].astype(jnp.float32)
            inverse = lax.rsqrt(jnp.mean(wide * wide, -1, keepdims=True) + 1e-6)
            a_s[rows, :] = (wide * inverse * gain).astype(jnp.bfloat16)

        if i:
            a_copy(c, i - 1).start()
    w_forward(0, 1)
    for j in range(1, STEPS):
        w_local(j)
    v_s[:, :, HEAD:, :] = jnp.ones((STEPS, 2, VR - HEAD, CHIP), jnp.bfloat16)
    a_copy(c, 3).start()
    for j in range(1, STEPS):
        w_sib(j)
    for r in range(2, CUT):
        w_forward(0, r)
    for i in range(4):
        a_copy(1 - c, i).wait_recv()
    w_forward(1, 0)

    def project(t):
        slot = lax.rem(t, 2)

        @pl.loop(0, CHIP // 1024)
        def _(m):
            rows = pl.ds(pl.multiple_of(m * 1024, 1024), 1024)
            got = _dot(a_s[rows, :], w_s[t], 1, 0)
            cos, sin = cos_s[rows, :], sin_s[rows, :]
            for g in range(G + 1):
                part = got[:, g * HEAD : (g + 1) * HEAD].astype(jnp.bfloat16).astype(jnp.float32)
                part = (part * cos + pltpu.roll(part, HEAD // 2, 1) * sin).astype(jnp.bfloat16)
                if g < G:
                    q_s[slot, g, rows, :] = part
                else:
                    k_s[t, chip, rows, :] = part
            v_s[t, chip, :HEAD, rows] = got[:, QC + HEAD :].T.astype(jnp.bfloat16)

    def kv_copies(t):
        k, v = k_s.at[t, 0], v_s.at[t, 0, :HEAD, :]
        device = (y, 2 * (1 - chip) + c)
        return remote(k, k, kv_send.at[t, 0], kv_recv.at[t, 0], device), remote(v, v, kv_send.at[t, 1], kv_recv.at[t, 1], device)

    def seen_place(half, j, core):
        return seen_s.at[pl.ds(pl.multiple_of(half * BQ, BQ), BQ), pl.ds(pl.multiple_of((2 * j + core) * QC, QC), QC)]

    def seen_send(j, half):
        return remote(st_s.at[lax.rem(j, 2), half], seen_place(half, j, c), so_send.at[j, half], so_recv.at[j, half], sib)

    def queries(iq):
        return pl.ds(pl.multiple_of(iq * BQ, BQ), BQ)

    def block(j, iq, half, at):
        here = pl.ds(pl.multiple_of(at * BK, BK), BK)
        keys = k_s[j, half, here, :]
        scores = [_dot(keys, q_s[lax.rem(j, 2), g, queries(iq), :], 1, 1) for g in range(G)]
        weights, keeps = [], []
        for g, sc in enumerate(scores):
            cols = slice(g * BQ, (g + 1) * BQ)
            old = top_s[iq, :, cols]
            top = jnp.maximum(old, sc.max(axis=0, keepdims=True))
            top_s[iq, :, cols] = top
            keeps.append(jnp.exp2((old - top) * e))
            weights.append(jnp.exp2((sc - top) * e).astype(jnp.bfloat16))
        values = v_s[j, half, :, here]
        for g, p in enumerate(weights):
            cols = slice(g * BQ, (g + 1) * BQ)
            mix_s[iq, :, cols] = mix_s[iq, :, cols] * keeps[g] + _dot(values, p, 1, 0)

    def diagonal(j, iq):
        here = pl.multiple_of(iq * BQ, BQ)
        strips = [(g, at) for g in range(G) for at in range(0, BQ, SQ)]
        scores = [_dot(k_s[j, chip, pl.ds(here, at + SQ), :],
                       q_s[lax.rem(j, 2), g, pl.ds(pl.multiple_of(here + at, SQ), SQ), :], 1, 1) for g, at in strips]
        weights = []
        for (g, at), sc in zip(strips, scores):
            cols = slice(g * BQ + at, g * BQ + at + SQ)
            ok = lax.broadcasted_iota(jnp.int32, sc.shape, 1) + at >= lax.broadcasted_iota(jnp.int32, sc.shape, 0)
            sc = jnp.where(ok, sc, HIDDEN)
            top = sc.max(axis=0, keepdims=True)
            top_s[iq, :, cols] = top
            weights.append(jnp.exp2((sc - top) * e).astype(jnp.bfloat16))
        for (g, at), p in zip(strips, weights):
            mix_s[iq, :, g * BQ + at : g * BQ + at + SQ] = _dot(v_s[j, chip, :, pl.ds(here, at + SQ)], p, 1, 0)

    def attend_own(j):
        @pl.loop(0, CHIP // BQ)
        def _(iq):
            for at, n in FORWARD_OWN:
                @pl.when((j == at // 4) & (iq == at % 4))
                def _():
                    wo_forward(n)

            diagonal(j, iq)

            @pl.loop(0, iq)
            def _(i):
                block(j, iq, chip, i)

            @pl.when((j == 0) & (iq == 2))
            def _():
                w_forward(1, 3)

    def attend_other(j):
        @pl.when(chip == 1)
        def _():
            for copy in kv_copies(j):
                copy.wait_recv()

        @pl.loop(0, CHIP // BQ)
        def _(iq):
            @pl.when((j < 2) & (iq > 0))
            def _():
                w_forward(j + 2, iq - 1)

            @pl.when((j < 2) & (iq == 3))
            def _():
                w_forward(j + 2, 3)

            for at, n in FORWARD:
                @pl.when((j == at // 4) & (iq == at % 4))
                def _():
                    wo_forward(n)

            @pl.when(j == 3)
            def _():
                wo_share(iq)

            @pl.when((j == 3) & (iq == 3))
            def _():
                for jj in range(STEPS):
                    for core in range(2):
                        for r in range(CUT):
                            here = place(jj, (other + core) * SHARD + y * HALF + r * PIECE, PIECE)
                            remote(here, here, yw_send.at[jj, core, r], yw_recv.at[jj, core, r], twin).wait_send()
                theirs = wof_ref.at[pl.ds(pl.multiple_of((s + 1 - 2 * c) * OWN, OWN), OWN), :]
                remote(theirs, theirs, swo_send, swo_recv, sib).wait_recv()
                fetch(0)

            @pl.loop(0, chip * (CHIP // BK))
            def _(i):
                block(j, iq, 0, i)

            outs = []
            for g in range(G):
                cols = slice(g * BQ, (g + 1) * BQ)
                total = mix_s[iq, HEAD : HEAD + 1, cols]
                outs.append((mix_s[iq, :HEAD, cols] * (1 / total)).T.astype(jnp.bfloat16))
            half = lax.rem(iq, 2)

            @pl.when(lax.div(iq, 2) == c)
            def _():
                for g, out in enumerate(outs):
                    seen_s[pl.ds(pl.multiple_of(half * BQ, BQ), BQ), pl.ds(pl.multiple_of((2 * j + c) * QC + g * HEAD, HEAD), HEAD)] = out

            @pl.when(lax.div(iq, 2) != c)
            def _():
                @pl.when(j >= 2)
                def _():
                    seen_send(j - 2, half).wait_send()

                for g, out in enumerate(outs):
                    st_s[lax.rem(j, 2), half, :, g * HEAD : (g + 1) * HEAD] = out
                seen_send(j, half).start()

    @pl.loop(0, STEPS + 1)
    def _(t):
        @pl.when(t < STEPS)
        def _():
            w_wait(t)
            project(t)

            @pl.when(chip == 0)
            def _():
                for copy in kv_copies(t):
                    copy.start()

            @pl.when(t == 0)
            def _():
                w_across(2)
                w_forward(1, 1)
                w_forward(1, 2)
                remote(wo_ref, wof_ref.at[pl.ds(pl.multiple_of(s * OWN, OWN), OWN), :], swo_send, swo_recv, sib).start()

            @pl.when(t == 1)
            def _():
                w_across(3)

            @pl.when(t == 2)
            def _():
                wo_across(0)

            @pl.when(t == 3)
            def _():
                for n in range(1, KP):
                    wo_across(n)

        @pl.when(t > 0)
        def _():
            attend_other(t - 1)

        @pl.when(t < STEPS)
        def _():
            attend_own(t)

    wo_forward(7)
    wo_forward(8)
    wo_share(4)
    for j in range(STEPS):
        for half in range(2):
            here = seen_place(half, j, 1 - c)
            remote(here, here, so_send.at[j, half], so_recv.at[j, half], sib).wait_recv()

    @pl.loop(0, KP)
    def _(n):
        @pl.when(n == 2)
        def _():
            wo_forward(9)

        @pl.when((n >= 3) & (n + 2 < KP))
        def _():
            wo_share(n + 2)

        @pl.when(n + 1 < KP)
        def _():
            fetch(n + 1)

        finish(n)

    for n in range(KP - 2, KP):
        y_copy(n).wait()
    mine = wof_ref.at[pl.ds(pl.multiple_of(s * OWN, OWN), OWN), :]
    remote(wo_ref, mine, swo_send, swo_recv, sib).wait_send()
    for i in range(4):
        a_copy(c, i).wait_send()
    for j in range(STEPS):
        here = place(j, s * SHARD, SHARD)
        remote(here, here, sw_send.at[j], sw_recv.at[j], sib).wait_send()
        for core in range(2):
            for r in range(CUT):
                here = place(j, s * SHARD + y * HALF + r * PIECE, PIECE)
                remote(here, here, xw_send.at[j, core, r], xw_recv.at[j, c, r], across(core)).wait_send()

        @pl.when(chip == 0)
        def _():
            for copy in kv_copies(j):
                copy.wait_send()

        if j >= 2:
            for half in range(2):
                seen_send(j, half).wait_send()
    for n in range(KP):
        for core in range(2):
            mine = wo_place(s, 2 * y + core, n)
            remote(mine, mine, wx_send.at[n, core], wx_recv.at[n, c], across(core)).wait_send()
            here = wo_place(other + core, 2 * y + c, n)
            remote(here, here, wy_send.at[n, core], wy_recv.at[n, core], twin).wait_send()
            remote(here, here, wsx_send.at[n, core], wsx_recv.at[n, core], sib).wait_send()
            here = wo_place(other + core, 2 * (1 - y) + c, n)
            remote(here, here, wsy_send.at[n, core], wsy_recv.at[n, core], sib).wait_send()


def _layer(x, gain, freq, wq, wk, wv, wo):
    dma = lambda *shape: pltpu.SemaphoreType.DMA(shape) if shape else pltpu.SemaphoreType.DMA
    hbm, vmem = pl.BlockSpec(memory_space=pl.ANY), pl.BlockSpec(memory_space=pltpu.VMEM)
    bf16, f32 = jnp.bfloat16, jnp.float32
    return pl.pallas_call(
        _kernel,
        out_shape=[jax.ShapeDtypeStruct((OWN, D), bf16), jax.ShapeDtypeStruct((4 * OWN, D), bf16)],
        in_specs=[hbm, vmem, vmem, hbm, hbm, hbm, hbm],
        out_specs=[hbm, hbm],
        scratch_shapes=[
            pltpu.VMEM((CHIP, D), bf16), pltpu.VMEM((STEPS, D, WC), bf16), pltpu.VMEM((STEPS, 2, CHIP, HEAD), bf16),
            pltpu.VMEM((STEPS, 2, VR, CHIP), bf16), pltpu.VMEM((2, G, CHIP, HEAD), bf16), pltpu.VMEM((2, 2, BQ, QC), bf16),
            pltpu.VMEM((OWN, 4 * OWN), bf16), pltpu.VMEM((2, OWN, NC), bf16),
            pltpu.VMEM((CHIP, HEAD), f32), pltpu.VMEM((CHIP, HEAD), f32), pltpu.VMEM((CHIP // BQ, 1, COLS), f32), pltpu.VMEM((CHIP // BQ, VR, COLS), f32),
            dma(4), dma(4), dma(4), dma(4), dma(4), dma(4), dma(4, 2, CUT), dma(4, 2, CUT), dma(4, 2, CUT), dma(4, 2, CUT), dma(4, 2), dma(4, 2),
            dma(4, 2), dma(4, 2), dma(2), dma(2), dma(2), dma(), dma(), dma(KP, 2), dma(KP, 2), dma(KP, 2), dma(KP, 2),
            dma(KP, 2), dma(KP, 2), dma(KP, 2), dma(KP, 2),
        ],
        compiler_params=pltpu.CompilerParams(collective_id=0, has_side_effects=True, vmem_limit_bytes=63 * 2**20),
        cost_estimate=pl.CostEstimate(flops=120 * 10**9, transcendentals=10**8, bytes_accessed=100 * 2**20),
    )(x, gain, freq, wq, wk, wv, wo)


def solution(mesh):
    def step(x, gain, wq, wk, wv, wo):
        half = HEAD // 2
        freq = np.float32(THETA) ** (-np.arange(half, dtype=np.float32) / np.float32(half))
        freq = jnp.asarray(np.concatenate([freq, freq])[None], jnp.float32)
        return _layer(x, gain, freq, wq, wk, wv, wo)[0]

    tokens, rows = P(("dp", "sp"), None), P("sp", None)
    return jax.shard_map(
        step,
        mesh=mesh,
        in_specs=(tokens, P(None), rows, rows, rows, rows),
        out_specs=tokens,
        check_vma=False,
    )
```

```python
import functools

import jax
import jax.numpy as jnp
import numpy as np
from jax import lax
from jax.experimental import pallas as pl
from jax.experimental.pallas import tpu as pltpu
from jax.sharding import PartitionSpec as P

HEAD = 128
THETA = 10000
NEG = -1e30
HIDDEN = 2 * NEG
LOG2E = 1.4426950408889634
D = 2560
OWN = 1024
CHIP = 2 * OWN
STEPS = 4
G = 4
QC = G * HEAD
WC = QC + 2 * HEAD
SHARD = D // 4
HALF = SHARD // 2
CUT = 4
PIECE = HALF // CUT
BQ = 512
BK = 512
COLS = G * BQ
SQ = 256
VR = HEAD + 16
NC = 256
KP = D // NC
FORWARD = ((9, 0), (10, 1), (11, 2), (12, 3), (13, 4), (14, 5), (15, 6))
FORWARD_OWN = ()
MESH = pl.DeviceIdType.MESH


def _dot(a, b, ca, cb):
    return lax.dot_general(a, b, (((ca,), (cb,)), ((), ())), preferred_element_type=jnp.float32)


def _kernel(x_ref, gain_ref, freq_ref, wq_ref, wk_ref, wv_ref, wo_ref, y_ref, wof_ref,
            a_s, w_s, k_s, v_s, q_s, st_s, seen_s, y_s, cos_s, sin_s, top_s, mix_s,
            lx, a_send, a_recv, lw, sw_send, sw_recv, xw_send, xw_recv, yw_send, yw_recv, kv_send, kv_recv,
            so_send, so_recv, tl, tx, ty, swo_send, swo_recv, wx_send, wx_recv, wy_send, wy_recv,
            wsx_send, wsx_recv, wsy_send, wsy_recv):
    y, s = lax.axis_index("dp"), lax.axis_index("sp")
    chip, c = lax.div(s, 2), lax.rem(s, 2)
    other = 2 * (1 - chip)
    sib = (y, s + 1 - 2 * c)
    across = lambda core: (y, other + core)
    twin = (1 - y, s)
    scale = HEAD**-0.5
    e = scale * LOG2E

    def remote(src, dst, send, recv, device):
        return pltpu.make_async_remote_copy(src_ref=src, dst_ref=dst, send_sem=send, recv_sem=recv, device_id=device, device_id_type=MESH)

    barrier = pltpu.get_barrier_semaphore()
    for device in (sib, across(0), across(1), twin):
        pl.semaphore_signal(barrier, inc=1, device_id=device, device_id_type=MESH)
    pl.semaphore_wait(barrier, 4)

    def pieces(core, j, row, n):
        h = 2 * j + core
        rows = pl.ds(row, n)
        return ((wq_ref.at[rows, pl.ds(pl.multiple_of(h * QC, QC), QC)], pl.ds(0, QC)),
                (wk_ref.at[rows, pl.ds(pl.multiple_of(h * HEAD, HEAD), HEAD)], pl.ds(QC, HEAD)),
                (wv_ref.at[rows, pl.ds(pl.multiple_of(h * HEAD, HEAD), HEAD)], pl.ds(QC + HEAD, HEAD)))

    def place(j, row, n):
        return w_s.at[j, pl.ds(pl.multiple_of(row, 16), n), :]

    def w_local(j):
        for src, cols in pieces(c, j, 0, SHARD):
            pltpu.make_async_copy(src, w_s.at[j, pl.ds(pl.multiple_of(s * SHARD, HALF), SHARD), cols], lw.at[j]).start()

    def w_sib(j):
        for src, cols in pieces(1 - c, j, 0, SHARD):
            remote(src, w_s.at[j, pl.ds(pl.multiple_of(s * SHARD, HALF), SHARD), cols], sw_send.at[j], sw_recv.at[j], sib).start()

    def w_across(j):
        for r in range(CUT):
            for core in range(2):
                row = pl.multiple_of(y * HALF + r * PIECE, 16)
                for src, cols in pieces(core, j, row, PIECE):
                    remote(src, w_s.at[j, pl.ds(pl.multiple_of(s * SHARD + y * HALF + r * PIECE, 16), PIECE), cols],
                           xw_send.at[j, core, r], xw_recv.at[j, c, r], across(core)).start()

    def w_forward(j, r):
        for core in range(2):
            here = place(j, (other + core) * SHARD + y * HALF + r * PIECE, PIECE)
            remote(here, here, xw_send.at[j, core, r], xw_recv.at[j, core, r], across(core)).wait_recv()
            remote(here, here, yw_send.at[j, core, r], yw_recv.at[j, core, r], twin).start()

    def w_wait(j):
        here = place(j, s * SHARD, SHARD)
        pltpu.make_async_copy(here, here, lw.at[j]).wait()
        here = place(j, (s + 1 - 2 * c) * SHARD, SHARD)
        remote(here, here, sw_send.at[j], sw_recv.at[j], sib).wait_recv()
        for core in range(2):
            for r in range(CUT):
                here = place(j, (other + core) * SHARD + (1 - y) * HALF + r * PIECE, PIECE)
                remote(here, here, yw_send.at[j, core, r], yw_recv.at[j, core, r], twin).wait_recv()

    def wo_place(owner, quarter, n):
        return wof_ref.at[pl.ds(pl.multiple_of(owner * OWN + quarter * 256, 256), 256), pl.ds(pl.multiple_of(n * NC, NC), NC)]

    def wo_across(n):
        for core in range(2):
            src = wo_ref.at[pl.ds(pl.multiple_of((2 * y + core) * 256, 256), 256), pl.ds(pl.multiple_of(n * NC, NC), NC)]
            remote(src, wo_place(s, 2 * y + core, n), wx_send.at[n, core], wx_recv.at[n, c], across(core)).start()

    def wo_forward(n):
        for core in range(2):
            here = wo_place(other + core, 2 * y + c, n)
            remote(here, here, wx_send.at[n, core], wx_recv.at[n, core], across(core)).wait_recv()
            remote(here, here, wy_send.at[n, core], wy_recv.at[n, core], twin).start()
            remote(here, here, wsx_send.at[n, core], wsx_recv.at[n, core], sib).start()

    def wo_share(n):
        for core in range(2):
            here = wo_place(other + core, 2 * (1 - y) + c, n)
            remote(here, here, wy_send.at[n, core], wy_recv.at[n, core], twin).wait_recv()
            remote(here, here, wsy_send.at[n, core], wsy_recv.at[n, core], sib).start()

    def fetch(n):
        for core in range(2):
            here = wo_place(other + core, 2 * y + 1 - c, n)
            remote(here, here, wsx_send.at[n, core], wsx_recv.at[n, core], sib).wait_recv()
            here = wo_place(other + core, 2 * (1 - y) + 1 - c, n)
            remote(here, here, wsy_send.at[n, core], wsy_recv.at[n, core], sib).wait_recv()
        slot = lax.rem(n, 2)
        cols = pl.ds(pl.multiple_of(n * NC, NC), NC)

        def take(src, core, half):
            dst = w_s.at[slot, pl.ds(pl.multiple_of(core * OWN, OWN), OWN), pl.ds(pl.multiple_of(half * NC, NC), NC)]
            pltpu.make_async_copy(src, dst, tl.at[slot]).start()

        take(wo_ref.at[:, cols], c, chip)
        take(wof_ref.at[pl.ds(pl.multiple_of((s + 1 - 2 * c) * OWN, OWN), OWN), cols], 1 - c, chip)
        for core in range(2):
            take(wof_ref.at[pl.ds(pl.multiple_of((other + core) * OWN, OWN), OWN), cols], core, 1 - chip)
        pltpu.make_async_copy(x_ref.at[:, cols], w_s.at[slot, :OWN, 2 * NC :], tx.at[slot]).start()

    def y_copy(n):
        return pltpu.make_async_copy(y_s.at[lax.rem(n, 2)], y_ref.at[:, pl.ds(pl.multiple_of(n * NC, NC), NC)], ty.at[lax.rem(n, 2)])

    def finish(n):
        slot = lax.rem(n, 2)
        here = w_s.at[slot, : 2 * OWN, : 2 * NC]
        pltpu.make_async_copy(here, here, tl.at[slot]).wait()
        here = w_s.at[slot, :OWN, 2 * NC :]
        pltpu.make_async_copy(here, here, tx.at[slot]).wait()

        @pl.when(n >= 2)
        def _():
            y_copy(n - 2).wait()

        for at in range(0, OWN, BQ):
            rows = slice(at, at + BQ)
            got = _dot(seen_s[rows, : 2 * OWN], w_s[slot, : 2 * OWN, :NC], 1, 0) + _dot(seen_s[rows, 2 * OWN :], w_s[slot, : 2 * OWN, NC : 2 * NC], 1, 0)
            y_s[slot, rows, :] = (w_s[slot, rows, 2 * NC :].astype(jnp.float32) + got).astype(jnp.bfloat16)
        y_copy(n).start()

    w_across(0)
    w_local(0)
    w_sib(0)
    w_across(1)
    for i in range(4):
        rows = pl.ds(pl.multiple_of(c * OWN + i * 256, 256), 256)
        pltpu.make_async_copy(x_ref.at[pl.ds(i * 256, 256), :], a_s.at[rows, :], lx.at[i]).start()

    @pl.loop(0, CHIP // 256)
    def _(i):
        rows = pl.ds(pl.multiple_of(i * 256, 256), 256)
        spot = (chip * CHIP + i * 256 + lax.broadcasted_iota(jnp.int32, (256, HEAD), 0)).astype(jnp.float32)
        angle = spot * freq_ref[...]
        cos_s[rows, :] = jnp.cos(angle)
        left = lax.broadcasted_iota(jnp.int32, (256, HEAD), 1) < HEAD // 2
        sin = jnp.sin(angle)
        sin_s[rows, :] = jnp.where(left, -sin, sin)

    w_forward(0, 0)
    gain = gain_ref[...].astype(jnp.float32)[None]

    def a_rows(core, i):
        return a_s.at[pl.ds(pl.multiple_of(core * OWN + i * 256, 256), 256), :]

    def a_copy(core, i):
        return remote(a_rows(core, i), a_rows(core, i), a_send.at[i], a_recv.at[i], sib)

    for i in range(4):
        pltpu.make_async_copy(x_ref.at[pl.ds(i * 256, 256), :], a_rows(c, i), lx.at[i]).wait()

        @pl.loop(0, 256 // 32)
        def _(r):
            rows = pl.ds(pl.multiple_of(c * OWN + i * 256 + r * 32, 32), 32)
            wide = a_s[rows, :].astype(jnp.float32)
            inverse = lax.rsqrt(jnp.mean(wide * wide, -1, keepdims=True) + 1e-6)
            a_s[rows, :] = (wide * inverse * gain).astype(jnp.bfloat16)

        if i:
            a_copy(c, i - 1).start()
    w_forward(0, 1)
    for j in range(1, STEPS):
        w_local(j)
    v_s[:, :, HEAD:, :] = jnp.ones((STEPS, 2, VR - HEAD, CHIP), jnp.bfloat16)
    a_copy(c, 3).start()
    for j in range(1, STEPS):
        w_sib(j)
    for r in range(2, CUT):
        w_forward(0, r)
    for i in range(4):
        a_copy(1 - c, i).wait_recv()
    w_forward(1, 0)

    def project(t):
        slot = lax.rem(t, 2)

        @pl.loop(0, CHIP // 1024)
        def _(m):
            rows = pl.ds(pl.multiple_of(m * 1024, 1024), 1024)
            got = _dot(a_s[rows, :], w_s[t], 1, 0)
            cos, sin = cos_s[rows, :], sin_s[rows, :]
            for g in range(G + 1):
                part = got[:, g * HEAD : (g + 1) * HEAD].astype(jnp.bfloat16).astype(jnp.float32)
                part = (part * cos + pltpu.roll(part, HEAD // 2, 1) * sin).astype(jnp.bfloat16)
                if g < G:
                    q_s[slot, g, rows, :] = part
                else:
                    k_s[t, chip, rows, :] = part
            v_s[t, chip, :HEAD, rows] = got[:, QC + HEAD :].T.astype(jnp.bfloat16)

            @pl.when((t == 0) & (m == 0))
            def _():
                w_forward(1, 1)

    def kv_copies(t, i):
        here = pl.ds(pl.multiple_of(i * BK, BK), BK)
        k, v = k_s.at[t, 0, here, :], v_s.at[t, 0, :HEAD, here]
        device = (y, 2 * (1 - chip) + c)
        return remote(k, k, kv_send.at[t, 0, i], kv_recv.at[t, 0, i], device), remote(v, v, kv_send.at[t, 1, i], kv_recv.at[t, 1, i], device)

    def seen_place(half, j, core):
        return seen_s.at[pl.ds(pl.multiple_of(half * BQ, BQ), BQ), pl.ds(pl.multiple_of((2 * j + core) * QC, QC), QC)]

    def seen_send(j, half):
        return remote(st_s.at[lax.rem(j, 2), half], seen_place(half, j, c), so_send.at[j, half], so_recv.at[j, half], sib)

    def queries(iq):
        return pl.ds(pl.multiple_of(iq * BQ, BQ), BQ)

    def block(j, iq, half, at):
        here = pl.ds(pl.multiple_of(at * BK, BK), BK)
        keys = k_s[j, half, here, :]
        scores = [_dot(keys, q_s[lax.rem(j, 2), g, queries(iq), :], 1, 1) for g in range(G)]
        weights, keeps = [], []
        for g, sc in enumerate(scores):
            cols = slice(g * BQ, (g + 1) * BQ)
            old = top_s[iq, :, cols]
            top = jnp.maximum(old, sc.max(axis=0, keepdims=True))
            top_s[iq, :, cols] = top
            keeps.append(jnp.exp2((old - top) * e))
            weights.append(jnp.exp2((sc - top) * e).astype(jnp.bfloat16))
        values = v_s[j, half, :, here]
        for g, p in enumerate(weights):
            cols = slice(g * BQ, (g + 1) * BQ)
            mix_s[iq, :, cols] = mix_s[iq, :, cols] * keeps[g] + _dot(values, p, 1, 0)

    def diagonal(j, iq):
        here = pl.multiple_of(iq * BQ, BQ)
        strips = [(g, at) for g in range(G) for at in range(0, BQ, SQ)]
        scores = [_dot(k_s[j, chip, pl.ds(here, at + SQ), :],
                       q_s[lax.rem(j, 2), g, pl.ds(pl.multiple_of(here + at, SQ), SQ), :], 1, 1) for g, at in strips]
        weights = []
        for (g, at), sc in zip(strips, scores):
            cols = slice(g * BQ + at, g * BQ + at + SQ)
            ok = lax.broadcasted_iota(jnp.int32, sc.shape, 1) + at >= lax.broadcasted_iota(jnp.int32, sc.shape, 0)
            sc = jnp.where(ok, sc, HIDDEN)
            top = sc.max(axis=0, keepdims=True)
            top_s[iq, :, cols] = top
            weights.append(jnp.exp2((sc - top) * e).astype(jnp.bfloat16))
        for (g, at), p in zip(strips, weights):
            mix_s[iq, :, g * BQ + at : g * BQ + at + SQ] = _dot(v_s[j, chip, :, pl.ds(here, at + SQ)], p, 1, 0)

    def attend_own(j):
        @pl.loop(0, CHIP // BQ)
        def _(iq):
            for at, n in FORWARD_OWN:
                @pl.when((j == at // 4) & (iq == at % 4))
                def _():
                    wo_forward(n)

            diagonal(j, iq)

            @pl.loop(0, iq)
            def _(i):
                block(j, iq, chip, i)

            @pl.when((j == 0) & (iq == 2))
            def _():
                w_forward(1, 3)

    def attend_other(j):
        @pl.loop(0, CHIP // BQ)
        def _(iq):
            @pl.when((j < 2) & (iq > 0))
            def _():
                w_forward(j + 2, iq - 1)

            @pl.when((j < 2) & (iq == 3))
            def _():
                w_forward(j + 2, 3)

            for at, n in FORWARD:
                @pl.when((j == at // 4) & (iq == at % 4))
                def _():
                    wo_forward(n)

            @pl.when(j == 3)
            def _():
                wo_share(iq)

            @pl.when((j == 3) & (iq == 3))
            def _():
                for jj in range(STEPS):
                    for core in range(2):
                        for r in range(CUT):
                            here = place(jj, (other + core) * SHARD + y * HALF + r * PIECE, PIECE)
                            remote(here, here, yw_send.at[jj, core, r], yw_recv.at[jj, core, r], twin).wait_send()
                theirs = wof_ref.at[pl.ds(pl.multiple_of((s + 1 - 2 * c) * OWN, OWN), OWN), :]
                remote(theirs, theirs, swo_send, swo_recv, sib).wait_recv()
                fetch(0)

            @pl.loop(0, chip * (CHIP // BK))
            def _(i):
                @pl.when(iq == 0)
                def _():
                    for copy in kv_copies(j, i):
                        copy.wait_recv()

                block(j, iq, 0, i)

            outs = []
            for g in range(G):
                cols = slice(g * BQ, (g + 1) * BQ)
                total = mix_s[iq, HEAD : HEAD + 1, cols]
                outs.append((mix_s[iq, :HEAD, cols] * (1 / total)).T.astype(jnp.bfloat16))
            half = lax.rem(iq, 2)

            @pl.when(lax.div(iq, 2) == c)
            def _():
                for g, out in enumerate(outs):
                    seen_s[pl.ds(pl.multiple_of(half * BQ, BQ), BQ), pl.ds(pl.multiple_of((2 * j + c) * QC + g * HEAD, HEAD), HEAD)] = out

            @pl.when(lax.div(iq, 2) != c)
            def _():
                @pl.when(j >= 2)
                def _():
                    seen_send(j - 2, half).wait_send()

                for g, out in enumerate(outs):
                    st_s[lax.rem(j, 2), half, :, g * HEAD : (g + 1) * HEAD] = out
                seen_send(j, half).start()

    @pl.loop(0, STEPS + 1)
    def _(t):
        @pl.when(t < STEPS)
        def _():
            w_wait(t)
            project(t)

            @pl.when(chip == 0)
            def _():
                for i in range(CHIP // BK):
                    for copy in kv_copies(t, i):
                        copy.start()

            @pl.when(t == 0)
            def _():
                w_across(2)
                w_forward(1, 2)
                remote(wo_ref, wof_ref.at[pl.ds(pl.multiple_of(s * OWN, OWN), OWN), :], swo_send, swo_recv, sib).start()

            @pl.when(t == 1)
            def _():
                w_across(3)

            @pl.when(t == 2)
            def _():
                for n in range(3):
                    wo_across(n)

            @pl.when(t == 3)
            def _():
                for n in range(3, KP):
                    wo_across(n)

        @pl.when(t > 0)
        def _():
            attend_other(t - 1)

        @pl.when(t < STEPS)
        def _():
            attend_own(t)

    wo_forward(7)
    wo_share(4)
    for j in range(STEPS):
        for half in range(2):
            here = seen_place(half, j, 1 - c)
            remote(here, here, so_send.at[j, half], so_recv.at[j, half], sib).wait_recv()

    @pl.loop(0, KP)
    def _(n):
        for at, piece in ((1, 8), (3, 9)):
            @pl.when(n == at)
            def _():
                wo_forward(piece)

        @pl.when((n >= 3) & (n + 2 < KP))
        def _():
            wo_share(n + 2)

        @pl.when(n + 1 < KP)
        def _():
            fetch(n + 1)

        finish(n)

    for n in range(KP - 2, KP):
        y_copy(n).wait()
    mine = wof_ref.at[pl.ds(pl.multiple_of(s * OWN, OWN), OWN), :]
    remote(wo_ref, mine, swo_send, swo_recv, sib).wait_send()
    for i in range(4):
        a_copy(c, i).wait_send()
    for j in range(STEPS):
        here = place(j, s * SHARD, SHARD)
        remote(here, here, sw_send.at[j], sw_recv.at[j], sib).wait_send()
        for core in range(2):
            for r in range(CUT):
                here = place(j, s * SHARD + y * HALF + r * PIECE, PIECE)
                remote(here, here, xw_send.at[j, core, r], xw_recv.at[j, c, r], across(core)).wait_send()

        @pl.when(chip == 0)
        def _():
            for i in range(CHIP // BK):
                for copy in kv_copies(j, i):
                    copy.wait_send()

        if j >= 2:
            for half in range(2):
                seen_send(j, half).wait_send()
    for n in range(KP):
        for core in range(2):
            mine = wo_place(s, 2 * y + core, n)
            remote(mine, mine, wx_send.at[n, core], wx_recv.at[n, c], across(core)).wait_send()
            here = wo_place(other + core, 2 * y + c, n)
            remote(here, here, wy_send.at[n, core], wy_recv.at[n, core], twin).wait_send()
            remote(here, here, wsx_send.at[n, core], wsx_recv.at[n, core], sib).wait_send()
            here = wo_place(other + core, 2 * (1 - y) + c, n)
            remote(here, here, wsy_send.at[n, core], wsy_recv.at[n, core], sib).wait_send()


def _layer(x, gain, freq, wq, wk, wv, wo):
    dma = lambda *shape: pltpu.SemaphoreType.DMA(shape) if shape else pltpu.SemaphoreType.DMA
    hbm, vmem = pl.BlockSpec(memory_space=pl.ANY), pl.BlockSpec(memory_space=pltpu.VMEM)
    bf16, f32 = jnp.bfloat16, jnp.float32
    return pl.pallas_call(
        _kernel,
        out_shape=[jax.ShapeDtypeStruct((OWN, D), bf16), jax.ShapeDtypeStruct((4 * OWN, D), bf16)],
        in_specs=[hbm, vmem, vmem, hbm, hbm, hbm, hbm],
        out_specs=[hbm, hbm],
        scratch_shapes=[
            pltpu.VMEM((CHIP, D), bf16), pltpu.VMEM((STEPS, D, WC), bf16), pltpu.VMEM((STEPS, 2, CHIP, HEAD), bf16),
            pltpu.VMEM((STEPS, 2, VR, CHIP), bf16), pltpu.VMEM((2, G, CHIP, HEAD), bf16), pltpu.VMEM((2, 2, BQ, QC), bf16),
            pltpu.VMEM((OWN, 4 * OWN), bf16), pltpu.VMEM((2, OWN, NC), bf16),
            pltpu.VMEM((CHIP, HEAD), f32), pltpu.VMEM((CHIP, HEAD), f32), pltpu.VMEM((CHIP // BQ, 1, COLS), f32), pltpu.VMEM((CHIP // BQ, VR, COLS), f32),
            dma(4), dma(4), dma(4), dma(4), dma(4), dma(4), dma(4, 2, CUT), dma(4, 2, CUT), dma(4, 2, CUT), dma(4, 2, CUT), dma(4, 2, CHIP // BK), dma(4, 2, CHIP // BK),
            dma(4, 2), dma(4, 2), dma(2), dma(2), dma(2), dma(), dma(), dma(KP, 2), dma(KP, 2), dma(KP, 2), dma(KP, 2),
            dma(KP, 2), dma(KP, 2), dma(KP, 2), dma(KP, 2),
        ],
        compiler_params=pltpu.CompilerParams(collective_id=0, has_side_effects=True, vmem_limit_bytes=63 * 2**20),
        cost_estimate=pl.CostEstimate(flops=120 * 10**9, transcendentals=10**8, bytes_accessed=100 * 2**20),
    )(x, gain, freq, wq, wk, wv, wo)


def solution(mesh):
    def step(x, gain, wq, wk, wv, wo):
        half = HEAD // 2
        freq = np.float32(THETA) ** (-np.arange(half, dtype=np.float32) / np.float32(half))
        freq = jnp.asarray(np.concatenate([freq, freq])[None], jnp.float32)
        return _layer(x, gain, freq, wq, wk, wv, wo)[0]

    tokens, rows = P(("dp", "sp"), None), P("sp", None)
    return jax.shard_map(
        step,
        mesh=mesh,
        in_specs=(tokens, P(None), rows, rows, rows, rows),
        out_specs=tokens,
        check_vma=False,
    )
```
